32 devices in a mesh: blk: 16 (over z, y, x), slab: 2 (over core).
Axes of the slice: x: 2, y: 2, z: 4, core: 2. Of those that a mesh axis runs over, the one named last changes fastest.
Arguments:
- sinogram: bfloat16 [32, 8, 2048], P('blk', 'slab'), parts along dimension 1, may hold values from -6 to 6
- jitter: bfloat16 [32], P('blk'), may hold values from -0.29882812 to 0.29882812
- shift: int32 [32], replicated, may hold values from -8 to 8
Outputs:
- image: float32 [32, 8, 2048], P('blk', 'slab'), parts along dimension 1
The draws below stay inside these ranges and needn't reach their ends.
There are 2 independent parts, one for each index of `slab`. The reference program is written for one: setup_inputs(seed, part) draws one part's arguments, and reference() takes and returns one part's arrays. A program takes and returns all parts, laid end to end along the dimension named above; an argument that names none is the same for every part. Nothing has to cross between parts.
All inputs are finite; a program needn't handle non-finite values.
Results may differ from the reference program's by a relative error of at most 0.0055.
Values may be sent and summed in bfloat16 or wider, within the bound.
A program may use at most 64 MiB of HBM per device.

```python
import math
import jax
import jax.numpy as jnp
from jax import lax

BINS = 2048
SLICES = 4
ANGLES = 32
NROWS = 32


def place_ends(array, rng, smallest, top_value):
    index_at = [jax.random.randint(jax.random.fold_in(rng, axis), (), 0, length) for axis, length in enumerate(array.shape)]
    main_axis = array.shape.index(max(array.shape))
    beside = index_at[:main_axis] + [(index_at[main_axis] + 1) % array.shape[main_axis]] + index_at[main_axis + 1:]
    return array.at[tuple(index_at)].set(smallest).at[tuple(beside)].set(top_value)


def block_scale(rng, shape, split, smallest, high):
    def one(dim, shards_of):
        heights = jax.random.uniform(jax.random.fold_in(jax.random.fold_in(rng, 6), dim), (shards_of,), jnp.float32, smallest / len(split), high / len(split))
        return jnp.repeat(jnp.exp(heights), shape[dim] // shards_of).reshape((-1,) + (1,) * (len(shape) - dim - 1))

    level = one(*split[0])
    for cut in split[1:]:
        level = level * one(*cut)
    return level


def bell_draw(key, shape, deviation, most, pieces=(), held_as=jnp.bfloat16):
    entries = deviation * jax.random.normal(key, shape, jnp.float32)
    if pieces:
        entries = entries * block_scale(key, shape, pieces, -0.22, 0.18)
    return jnp.clip(entries, -most, most).astype(held_as)


def setup_inputs(seed: int = 0, part: int = 0) -> dict:
    splits = jax.random.split(jax.random.key(seed), 4)
    part_keys = jax.random.split(jax.random.fold_in(splits[3], part), 4)
    return {
        "sinogram": bell_draw(part_keys[0], (ANGLES, SLICES, BINS), 1.0, 6.0, ((0, 16),)),
        "jitter": jnp.clip(jax.random.uniform(splits[1], (ANGLES,), jnp.float32, -0.29882812, 0.29882812) * block_scale(splits[1], (ANGLES,), ((0, 16),), -0.4, 0.0), -0.29882812, 0.29882812).astype(jnp.bfloat16),
        "shift": place_ends(jax.random.randint(splits[2], (ANGLES,), -8, 9), jax.random.fold_in(splits[2], 1), -8, 8).astype(jnp.int32),
    }


def ramp_matrix(bins):
    offsets = jnp.arange(bins, dtype=jnp.int32)[None, :] - jnp.arange(bins, dtype=jnp.int32)[:, None]
    safe = jnp.where(offsets == 0, 1, offsets).astype(jnp.float32)
    odd_part = jnp.where(offsets % 2 != 0, -1.0 / (math.pi ** 2 * safe * safe), jnp.float32(0.0))
    kernel = jnp.where(offsets == 0, jnp.float32(0.25), odd_part)
    return kernel.astype(jnp.bfloat16)

def reference(sinogram, jitter, shift):
    ramp = ramp_matrix(BINS)
    jit_vals = jitter.astype(jnp.float32)
    weight = (1.0 + (jnp.roll(jit_vals, -1) - jnp.roll(jit_vals, 1)) * 1.5) * (4.0 / math.sqrt(ANGLES))
    flat = jnp.dot(sinogram.reshape(ANGLES * SLICES, BINS), ramp, preferred_element_type=jnp.float32)
    filtered = (flat.reshape(ANGLES, SLICES, BINS) * weight[:, None, None]).astype(jnp.bfloat16)
    padding = BINS // 4 + 192
    padded = jnp.pad(filtered, ((0, 0), (0, 0), (padding, padding))).astype(jnp.float32)
    theta = (jnp.arange(ANGLES, dtype=jnp.float32) + jit_vals) * math.pi / ANGLES
    cosine = jnp.cos(theta)
    sine_part = jnp.sin(theta)
    center_bin = (BINS - 1) / 2 + shift.astype(jnp.float32)
    coords_x = jnp.arange(BINS, dtype=jnp.float32) - (BINS - 1) / 2

    def one_row(row):
        row_pos = row.astype(jnp.float32) - (NROWS - 1) / 2
        coords = coords_x[None, :] * cosine[:, None] + row_pos * sine_part[:, None] + center_bin[:, None]
        lower = jnp.floor(coords)
        upper = lower + 1.0
        w_lower = jnp.maximum(0.0, 1.0 - jnp.abs(lower - coords)).astype(jnp.bfloat16).astype(jnp.float32)
        w_upper = jnp.maximum(0.0, 1.0 - jnp.abs(upper - coords)).astype(jnp.bfloat16).astype(jnp.float32)
        low_idx = lower.astype(jnp.int32) + padding
        idx_lo = jnp.broadcast_to(low_idx[:, None, :], (ANGLES, SLICES, BINS))
        f_lower = jnp.take_along_axis(padded, idx_lo, axis=2)
        f_upper = jnp.take_along_axis(padded, idx_lo + 1, axis=2)
        return lax.optimization_barrier(jnp.sum(f_lower * w_lower[:, None, :] + f_upper * w_upper[:, None, :], axis=0))
    return lax.map(one_row, jnp.arange(NROWS, dtype=jnp.int32))
```

```python
import functools
import math

import jax
import jax.numpy as jnp
import numpy as np
from jax import lax
from jax.experimental import pallas as pl
from jax.experimental.pallas import tpu as pltpu
from jax.sharding import PartitionSpec as P

LANES = 128
SUBS = 8
BLOCK = 256
PLANE = 4
STEP = 64
JITTER = 0.29882812
SHIFT = 8
MESH = pl.DeviceIdType.MESH


def ramp_slab(bins):
    nb = bins // BLOCK
    column = np.arange(BLOCK, dtype=np.int32)
    order = np.concatenate([column[0::2], column[1::2]])
    starts = (np.arange(2 * nb - 1, dtype=np.int32) - (nb - 1)) * BLOCK
    cols = (starts[:, None] + order[None, :]).reshape(-1)
    offsets = cols[None, :] - column[:, None]
    safe = np.where(offsets == 0, 1, offsets).astype(np.float32)
    odd_part = np.where(
        offsets % 2 != 0, np.float32(-1.0) / (np.float32(math.pi**2) * safe * safe), np.float32(0)
    )
    return np.where(offsets == 0, np.float32(0.25), odd_part).astype(jnp.bfloat16)


def window_base(width, ang_dev, rows_dev, bins):
    depth = width // PLANE
    angles, nrows = width * ang_dev, width * rows_dev
    nblocks, per = bins // LANES, PLANE * ang_dev
    groups = depth * rows_dev // SUBS
    half = (bins - 1) / 2
    me = np.arange(width)
    z, q = me // PLANE, me % PLANE
    a = z[:, None] * per + np.arange(per)[None, :]
    theta = (a[..., None] + np.linspace(-JITTER, JITTER, 9)) * math.pi / angles
    zs = np.arange(groups)[:, None] * (SUBS // rows_dev) + np.array([0, SUBS // rows_dev - 1])
    rows = (zs[None] * PLANE + q[:, None, None]) * rows_dev + np.array([0, rows_dev - 1])
    y = rows - (nrows - 1) / 2
    x = np.arange(nblocks)[:, None] * LANES + np.array([0, LANES - 1]) - half
    u = (
        x[None, None, :, None, :, None, None] * np.cos(theta)[:, :, None, None, None, None, :]
        + y[:, None, None, :, None, :, None] * np.sin(theta)[:, :, None, None, None, None, :]
        + half
    )
    low = np.floor(u.min(axis=(4, 5, 6)) - 0.25).astype(np.int32)
    high = u.max(axis=(4, 5, 6)) + 0.25
    assert (high - low).max() + STEP < 2 * LANES
    assert low.min() - SHIFT >= -STEP and low.max() + SHIFT < bins + STEP
    return (low + STEP).reshape(width, 1, per * nblocks * groups)


def lane_gather(x, index):
    dims = lax.GatherDimensionNumbers(
        offset_dims=(),
        collapsed_slice_dims=(1,),
        start_index_map=(1,),
        operand_batching_dims=(0,),
        start_indices_batching_dims=(0,),
    )
    return lax.gather(
        x, index[..., None], dims, (1, 1), mode=lax.GatherScatterMode.PROMISE_IN_BOUNDS
    )


def kernel(
    width,
    jit_hbm,
    shift_hbm,
    sino_hbm,
    slab_hbm,
    base_hbm,
    out_ref,
    jit_ref,
    shift_ref,
    sino_ref,
    slab,
    base,
    chunks,
    jmsg,
    jall,
    tab,
    acc,
    fin,
    snd,
    rcv,
    lsem,
    sj,
    rj,
    s1,
    r1,
    s2,
    r2,
):
    me = lax.axis_index("blk")
    ang_dev, slices, bins = sino_ref.shape
    rows_dev = out_ref.shape[0]
    angles = width * ang_dev
    nrows = width * rows_dev
    nblocks = bins // LANES
    nspans = bins // BLOCK
    depth = width // PLANE
    per = PLANE * ang_dev
    groups = acc.shape[0]
    zper = SUBS // rows_dev
    z, q = me // PLANE, me % PLANE
    half = (bins - 1) / 2

    def remote(src, dst, send, recv, dev):
        return pltpu.make_async_remote_copy(
            src_ref=src,
            dst_ref=dst,
            send_sem=send,
            recv_sem=recv,
            device_id={"blk": dev},
            device_id_type=MESH,
        )

    loads = [
        pltpu.make_async_copy(src, dst, lsem.at[i])
        for i, (src, dst) in enumerate(
            [
                (jit_hbm, jit_ref),
                (sino_hbm, sino_ref),
                (slab_hbm, slab),
                (shift_hbm, shift_ref),
                (base_hbm.at[me], base),
            ]
        )
    ]
    for load in loads:
        load.start()

    barrier = pltpu.get_barrier_semaphore()

    @pl.loop(1, width)
    def _(i):
        pl.semaphore_signal(
            barrier, inc=1, device_id={"blk": (me + i) % width}, device_id_type=MESH
        )

    def peer(d):
        qx, qy = q % 2, q // 2
        return z * PLANE + (qx + d % 2) % 2 + 2 * ((qy + d // 2) % 2)

    def jplane(d):
        return remote(jmsg, jall.at[d], sj.at[d - 1], rj.at[d - 1], peer(d))

    def jnext(p):
        return remote(
            jmsg, jall.at[PLANE], sj.at[PLANE - 1 + p], rj.at[PLANE - 1],
            (z + 1) % depth * PLANE + p,
        )

    def jprev(p):
        return remote(
            jmsg, jall.at[PLANE + 1], sj.at[PLANE - 1 + p], rj.at[PLANE],
            (z + depth - 1) % depth * PLANE + p,
        )

    def share(d):
        return remote(chunks.at[q], chunks.at[q], s1.at[d - 1], r1.at[d - 1], peer(d))

    def give(zt):
        return remote(snd.at[zt], rcv.at[z], s2.at[zt], r2.at[z], zt * PLANE + q)

    def take(zs):
        return remote(snd.at[zs], rcv.at[zs], s2.at[zs], r2.at[zs], zs * PLANE + q)

    lane = lax.broadcasted_iota(jnp.int32, (SUBS, LANES), 1)
    sub = lax.broadcasted_iota(jnp.int32, (SUBS, LANES), 0)
    lanef = lane.astype(jnp.float32)
    zero = jnp.zeros((SUBS, LANES), jnp.float32)
    last = tab.shape[1] - 1
    for p in range(2):
        tab[p, last] = zero
    for g in range(groups):
        for s in range(slices):
            for b in range(nblocks):
                acc[g, s, b] = zero

    loads[0].wait()
    mine = (lane[:1] % angles) - me * ang_dev
    msg = jnp.zeros((1, LANES), jnp.float32)
    for i in range(ang_dev):
        msg = jnp.where(mine == i, jit_ref[0:1, i : i + 1].astype(jnp.float32), msg)
    jmsg[...] = msg
    jall[0] = msg

    loads[1].wait()
    flat = jnp.concatenate(
        [sino_ref[i].astype(jnp.float32) for i in range(ang_dev)], axis=0
    )
    lhs = jnp.concatenate(
        [flat[:, i * BLOCK : (i + 1) * BLOCK] for i in range(nspans)], axis=0
    ).astype(jnp.bfloat16)
    loads[2].wait()
    total = [None] * nspans
    for d in range(2 * nspans - 1):
        prod = jnp.dot(
            lhs, slab[:, d * BLOCK : (d + 1) * BLOCK], preferred_element_type=jnp.float32
        )
        for i in range(nspans):
            j = d - (nspans - 1) + i
            if 0 <= j < nspans:
                piece = prod[i * SUBS : (i + 1) * SUBS]
                total[j] = piece if total[j] is None else total[j] + piece
    for t in range(nspans):
        chunks[q, :, t * LANES : (t + 1) * LANES] = jnp.concatenate(
            [total[t][:, :LANES], total[t][:, LANES:]], axis=0
        ).astype(jnp.bfloat16)

    pl.semaphore_wait(barrier, width - 1)

    for d in (3, 1, 2):
        jplane(d).start()

    @pl.when(q == PLANE - 1)
    def _():
        for p in range(PLANE):
            jnext(p).start()

    @pl.when(q == 0)
    def _():
        for p in range(PLANE):
            jprev(p).start()

    for d in (3, 1, 2):
        share(d).start()

    for d in range(1, PLANE):
        jplane(d).wait_recv()
    jnext(0).wait_recv()
    jprev(0).wait_recv()
    loads[3].wait()
    loads[4].wait()

    jit = jall[0]
    for i in range(1, PLANE + 2):
        jit = jit + jall[i]
    jit = jnp.broadcast_to(jit, (SUBS, LANES))
    ahead = pltpu.roll(jit, LANES - 1, 1)
    behind = pltpu.roll(jit, 1, 1)
    weight = (1.0 + (ahead - behind) * 1.5) * (4.0 / math.sqrt(angles))
    theta = ((lane % angles).astype(jnp.float32) + jit) * math.pi / angles
    cosine = jnp.cos(theta) * 0.5
    sine = jnp.sin(theta) * 0.5
    low_half = sub < slices
    low_row = sub < zper
    ypos = []
    for g in range(groups):
        row = ((sub % zper + g * zper) * PLANE + q) * rows_dev + sub // zper
        ypos.append(row.astype(jnp.float32) - (nrows - 1) / 2)

    @pl.loop(0, PLANE)
    def _(d):
        @pl.when(d > 0)
        def _():
            share(d).wait_recv()

        pc = peer(d)
        qc = pc - z * PLANE
        first = pc * ang_dev
        wts = lane_gather(weight, first + jnp.where(low_half, 0, 1))
        tiles = []
        for t in range(nspans):
            both = chunks[qc, :, t * LANES : (t + 1) * LANES].astype(jnp.float32)
            tiles.append((both[:SUBS] * wts, both[SUBS:] * wts))
        for p in range(2):
            for t in range(nspans):
                tab[p, 4 * t + 1] = tiles[t][p]
            for j in range(1, 4):
                cut = LANES - 32 * j
                turned = [pltpu.roll(tiles[t][p], cut, 1) for t in range(nspans)] + [zero]
                for t in range(nspans):
                    tab[p, 4 * t + j + 1] = jnp.where(lane < cut, turned[t], turned[t + 1])
                if j == 3:
                    tab[p, 0] = jnp.where(lane < cut, 0.0, turned[0])

        spans = []
        for i in range(ang_dev):
            pick = jnp.full((SUBS, LANES), first + i, jnp.int32)
            cosb, sinb = lane_gather(cosine, pick), lane_gather(sine, pick)
            spans.append((cosb, [lanef * cosb + ypos[g] * sinb for g in range(groups)]))
        for b in range(nblocks):
            for g in range(groups):
                sums = [None] * slices
                for i in range(ang_dev):
                    moved = shift_ref[first + i]
                    slot = base[0, ((qc * ang_dev + i) * nblocks + b) * groups + g]
                    slot = lax.shift_right_arithmetic(slot + moved, 6)
                    offset = (moved - slot * STEP).astype(jnp.float32) * 0.5
                    cosb, part = spans[i]
                    h = cosb * (b * LANES - half) + part[g] + (offset + (half + STEP) * 0.5)
                    odd = h.astype(jnp.int32)
                    even = (h + 0.5).astype(jnp.int32)
                    frac = jnp.abs(h - even.astype(jnp.float32)) * 2.0
                    evens, odds = [], []
                    for s in range(slices):
                        r = i * slices + s
                        line = jnp.broadcast_to(tab[0, slot, r : r + 1], (SUBS, LANES))
                        evens.append(lane_gather(line, even))
                    for s in range(slices):
                        r = i * slices + s
                        line = jnp.broadcast_to(tab[1, slot, r : r + 1], (SUBS, LANES))
                        odds.append(lane_gather(line, odd))
                    for s in range(slices):
                        got = evens[s] + frac * (odds[s] - evens[s])
                        sums[s] = got if sums[s] is None else sums[s] + got
                for s in range(slices):
                    acc[g, s, b] += sums[s]

    pos = sub % zper
    for g in range(groups):
        for t in range(nblocks // 2):
            out = [[], [], [], []]
            for b in (2 * t, 2 * t + 1):
                v = [acc[g, s, b] for s in range(slices)]
                w = [None] * 4
                for s in range(2):
                    w[s] = jnp.where(pos < 2, v[s], pltpu.roll(v[s + 2], 2, 0))
                    w[s + 2] = jnp.where(pos < 2, pltpu.roll(v[s], SUBS - 2, 0), v[s + 2])
                for s in (0, 2):
                    lo = jnp.where(pos % 2 < 1, w[s], pltpu.roll(w[s + 1], 1, 0))
                    hi = jnp.where(pos % 2 < 1, pltpu.roll(w[s], SUBS - 1, 0), w[s + 1])
                    for n, val in ((s, lo), (s + 1, hi)):
                        fin[g * zper + n, b] = val
                        out[n].append(val)
            for n in range(4):
                snd[g * zper + n, :, t * LANES : (t + 1) * LANES] = jnp.concatenate(
                    out[n], axis=0
                ).astype(jnp.bfloat16)

    @pl.loop(0, depth)
    def _(zt):
        @pl.when(zt != z)
        def _():
            give(zt).start()

    @pl.loop(1, depth)
    def _(k):
        take((z + k) % depth).wait_recv()

    for t in range(nblocks // 2):
        sums = [fin[z, 2 * t], fin[z, 2 * t + 1]]
        for k in range(1, depth):
            both = rcv[(z + k) % depth, :, t * LANES : (t + 1) * LANES].astype(jnp.float32)
            sums = [sums[0] + both[:SUBS], sums[1] + both[SUBS:]]
        for j in range(2):
            b = 2 * t + j
            for r in range(rows_dev):
                out_ref[r, :, b * LANES : (b + 1) * LANES] = sums[j][r * slices : (r + 1) * slices]

    for d in range(1, PLANE):
        jplane(d).wait_send()
        share(d).wait_send()

    @pl.when(q == PLANE - 1)
    def _():
        for p in range(PLANE):
            jnext(p).wait_send()

    @pl.when(q == 0)
    def _():
        for p in range(PLANE):
            jprev(p).wait_send()

    @pl.loop(1, depth)
    def _(k):
        give((z + k) % depth).wait_send()


def body(sinogram, jitter, shift):
    width = lax.axis_size("blk")
    ang_dev, slices, bins = sinogram.shape
    angles = shift.shape[0]
    rows_dev = SUBS // slices
    depth = width // PLANE
    assert ang_dev == 2 and rows_dev == 2 and slices == 4 and LANES % angles == 0
    assert width % (PLANE * 4) == 0 and bins % (2 * BLOCK) == 0
    groups = depth * rows_dev // SUBS
    nblocks = bins // LANES
    anywhere = pl.BlockSpec(memory_space=pl.ANY)
    dma = pltpu.SemaphoreType.DMA
    slab = jnp.asarray(ramp_slab(bins))
    base = jnp.asarray(window_base(width, ang_dev, rows_dev, bins))
    return pl.pallas_call(
        functools.partial(kernel, width),
        out_shape=pltpu.VMEM((rows_dev, slices, bins), jnp.float32),
        in_specs=[anywhere] * 5,
        out_specs=pl.BlockSpec(memory_space=pltpu.VMEM),
        scratch_shapes=[
            pltpu.VMEM((1, ang_dev), jnp.bfloat16),
            pltpu.SMEM((angles,), jnp.int32),
            pltpu.VMEM((ang_dev, slices, bins), jnp.bfloat16),
            pltpu.VMEM(slab.shape, jnp.bfloat16),
            pltpu.SMEM(base.shape[1:], jnp.int32),
            pltpu.VMEM((PLANE, 2 * SUBS, bins // 2), jnp.bfloat16),
            pltpu.VMEM((1, LANES), jnp.float32),
            pltpu.VMEM((PLANE + 2, 1, LANES), jnp.float32),
            pltpu.VMEM((2, bins // STEP + 2, SUBS, LANES), jnp.float32),
            pltpu.VMEM((groups, slices, nblocks, SUBS, LANES), jnp.float32),
            pltpu.VMEM((depth, nblocks, SUBS, LANES), jnp.float32),
            pltpu.VMEM((depth, 2 * SUBS, bins // 2), jnp.bfloat16),
            pltpu.VMEM((depth, 2 * SUBS, bins // 2), jnp.bfloat16),
            dma((5,)),
            dma((2 * PLANE - 1,)),
            dma((PLANE + 1,)),
            dma((PLANE - 1,)),
            dma((PLANE - 1,)),
            dma((depth,)),
            dma((depth,)),
        ],
        compiler_params=pltpu.CompilerParams(collective_id=0, has_side_effects=True),
    )(jitter.reshape(1, ang_dev), shift, sinogram, slab, base)


def solution(mesh):
    in_specs = (P("blk", "slab", None), P("blk"), P())
    out_specs = P("blk", "slab", None)
    return jax.shard_map(body, mesh=mesh, in_specs=in_specs, out_specs=out_specs, check_vma=False)
```

```python
import functools
import math

import jax
import jax.numpy as jnp
import numpy as np
from jax import lax
from jax.experimental import pallas as pl
from jax.experimental.pallas import tpu as pltpu
from jax.sharding import PartitionSpec as P

LANES = 128
SUBS = 8
BLOCK = 256
PLANE = 4
STEP = 64
JITTER = 0.29882812
SHIFT = 8
PIECES = 4
PARTS = 2
MESH = pl.DeviceIdType.MESH


def ramp_slab(bins):
    span = bins // 2
    first = -(span - LANES)
    offset = np.arange(first, span, dtype=np.int32)[None, :] - np.arange(LANES, dtype=np.int32)[:, None]
    both = 2 * np.stack([offset, offset - 1]) + 1
    safe = both.astype(np.float32)
    slab = (np.float32(-1.0) / (np.float32(math.pi**2) * safe * safe)).astype(jnp.bfloat16)
    tiles = slab.reshape(2, LANES, -1, LANES)
    return np.ascontiguousarray(tiles.transpose(2, 0, 1, 3))


def window_base(width, ang_dev, rows_dev, bins):
    depth = width // PLANE
    angles, nrows = width * ang_dev, width * rows_dev
    nblocks, per = bins // LANES, PLANE * ang_dev
    groups = depth * rows_dev // SUBS
    half = (bins - 1) / 2
    me = np.arange(width)
    z, q = me // PLANE, me % PLANE
    a = z[:, None] * per + np.arange(per)[None, :]
    theta = (a[..., None] + np.linspace(-JITTER, JITTER, 9)) * math.pi / angles
    zs = np.arange(groups)[:, None] * (SUBS // rows_dev) + np.array([0, SUBS // rows_dev - 1])
    rows = (zs[None] * PLANE + q[:, None, None]) * rows_dev + np.array([0, rows_dev - 1])
    y = rows - (nrows - 1) / 2
    x = np.arange(nblocks)[:, None] * LANES + np.array([0, LANES - 1]) - half
    u = (
        x[None, None, :, None, :, None, None] * np.cos(theta)[:, :, None, None, None, None, :]
        + y[:, None, None, :, None, :, None] * np.sin(theta)[:, :, None, None, None, None, :]
        + half
    )
    low = np.floor(u.min(axis=(4, 5, 6)) - 0.25).astype(np.int32)
    high = u.max(axis=(4, 5, 6)) + 0.25
    assert (high - low).max() + STEP < 2 * LANES
    assert low.min() - SHIFT >= -STEP and low.max() + SHIFT < bins + STEP
    return (low + STEP).reshape(width, 1, per * nblocks * groups)


def lane_gather(x, index):
    dims = lax.GatherDimensionNumbers(
        offset_dims=(),
        collapsed_slice_dims=(1,),
        start_index_map=(1,),
        operand_batching_dims=(0,),
        start_indices_batching_dims=(0,),
    )
    return lax.gather(
        x, index[..., None], dims, (1, 1), mode=lax.GatherScatterMode.PROMISE_IN_BOUNDS
    )


def kernel(
    width,
    jit_hbm,
    shift_hbm,
    sino_hbm,
    slab_hbm,
    base_hbm,
    out_ref,
    jit_ref,
    shift_ref,
    sino_ref,
    slab,
    base,
    chunks,
    msgs,
    tab,
    acc,
    fin,
    snd,
    rcv,
    lsem,
    wsem,
    sj,
    rj,
    s1,
    r1,
    s2,
    r2,
):
    me = lax.axis_index("blk")
    ang_dev, slices, bins = sino_ref.shape
    rows_dev = out_ref.shape[0]
    angles = width * ang_dev
    nrows = width * rows_dev
    nblocks = bins // LANES
    nspans = bins // BLOCK
    depth = width // PLANE
    groups = acc.shape[0]
    zper = SUBS // rows_dev
    z, q = me // PLANE, me % PLANE
    half = (bins - 1) / 2

    def remote(src, dst, send, recv, dev):
        return pltpu.make_async_remote_copy(
            src_ref=src,
            dst_ref=dst,
            send_sem=send,
            recv_sem=recv,
            device_id={"blk": dev},
            device_id_type=MESH,
        )

    loads = [
        pltpu.make_async_copy(src, dst, lsem.at[i])
        for i, (src, dst) in enumerate(
            [
                (jit_hbm, jit_ref),
                (sino_hbm, sino_ref),
                (shift_hbm, shift_ref),
                (base_hbm.at[me], base),
            ]
        )
    ]
    kblocks = bins // 2 // BLOCK
    ntiles = slab.shape[0]
    cuts = [0]
    for piece in range(PIECES):
        cuts.append(min(ntiles, 1 + 2 * -(-(2 * kblocks - 1) * (piece + 1) // PIECES)))
    weights = [
        pltpu.make_async_copy(
            slab_hbm.at[cuts[n] : cuts[n + 1]], slab.at[cuts[n] : cuts[n + 1]], wsem.at[n]
        )
        for n in range(PIECES)
    ]
    for load in loads[:2] + weights + loads[2:]:
        load.start()

    barrier = pltpu.get_barrier_semaphore()

    @pl.loop(1, width)
    def _(i):
        pl.semaphore_signal(
            barrier, inc=1, device_id={"blk": (me + i) % width}, device_id_type=MESH
        )

    def peer(d):
        qx, qy = q % 2, q // 2
        return z * PLANE + (qx + d % 2) % 2 + 2 * ((qy + d // 2) % 2)

    jrow = msgs.at[0, SUBS : 2 * SUBS]

    def jplane(d):
        return remote(msgs.at[0], msgs.at[d], sj.at[d - 1], rj.at[d - 1], peer(d))

    def jnext(p):
        return remote(
            jrow, msgs.at[PLANE, SUBS : 2 * SUBS], sj.at[PLANE - 1 + p], rj.at[PLANE - 1],
            (z + 1) % depth * PLANE + p,
        )

    def jprev(p):
        return remote(
            jrow, msgs.at[PLANE + 1, SUBS : 2 * SUBS], sj.at[PLANE - 1 + p], rj.at[PLANE],
            (z + depth - 1) % depth * PLANE + p,
        )

    def share(d):
        return remote(chunks.at[0], chunks.at[d], s1.at[d - 1], r1.at[d - 1], peer(d))

    def give(zt, part):
        return remote(
            snd.at[part, zt], rcv.at[part, z], s2.at[part, zt], r2.at[part, z], zt * PLANE + q
        )

    def take(zs, part):
        return remote(
            snd.at[part, zs], rcv.at[part, zs], s2.at[part, zs], r2.at[part, zs], zs * PLANE + q
        )

    lane = lax.broadcasted_iota(jnp.int32, (SUBS, LANES), 1)
    sub = lax.broadcasted_iota(jnp.int32, (SUBS, LANES), 0)
    lanef = lane.astype(jnp.float32)
    tab[tab.shape[0] - 1] = jnp.zeros((SUBS, LANES), jnp.int32)

    loads[0].wait()
    mine = (lane % angles) - me * ang_dev
    msg = jnp.zeros((SUBS, LANES), jnp.float32)
    for i in range(ang_dev):
        msg = jnp.where(mine == i, jit_ref[0:1, i : i + 1].astype(jnp.float32), msg)
    msgs[0, SUBS : 2 * SUBS] = msg

    loads[1].wait()
    flat = jnp.concatenate(
        [sino_ref[i].astype(jnp.float32) for i in range(ang_dev)], axis=0
    )
    tiles = [flat[:, b * LANES : (b + 1) * LANES] for b in range(nblocks)]
    top = jnp.abs(tiles[0])
    for tile in tiles[1:]:
        top = jnp.maximum(top, jnp.abs(tile))
    top = jnp.broadcast_to(jnp.max(top, axis=1, keepdims=True), (SUBS, LANES))
    msgs[0, :SUBS] = jnp.maximum(top, 1e-30) * (0.51 / 32700)

    pl.semaphore_wait(barrier, width - 1)

    for d in (3, 1, 2):
        jplane(d).start()

    @pl.when(q == PLANE - 1)
    def _():
        for p in range(PLANE):
            jnext(p).start()

    @pl.when(q == 0)
    def _():
        for p in range(PLANE):
            jprev(p).start()

    split = []
    for p in range(2):
        index = (2 * lane + p) % LANES
        picked = [lane_gather(tile, index) for tile in tiles]
        split.append(
            [
                jnp.where(lane < LANES // 2, picked[2 * t], picked[2 * t + 1])
                for t in range(nspans)
            ]
        )
    lhs = [
        jnp.concatenate(
            [jnp.concatenate([part[2 * k], part[2 * k + 1]], axis=1) for k in range(kblocks)],
            axis=0,
        ).astype(jnp.bfloat16)
        for part in split
    ]
    total = [
        [split[1 - p][t] * 0.25 for t in range(nspans)] for p in range(2)
    ]
    ready = 0
    for d in range(2 * kblocks - 1):
        while cuts[ready] < 2 * d + 3:
            weights[ready].wait()
            ready += 1
        for p in range(2):
            up = jnp.concatenate([slab[2 * d + 1, p], slab[2 * d + 2, p]], axis=1)
            down = jnp.concatenate([slab[2 * d, p], slab[2 * d + 1, p]], axis=1)
            prod = jnp.dot(
                lhs[p], jnp.concatenate([up, down], axis=0), preferred_element_type=jnp.float32
            )
            for i in range(kblocks):
                j = d - (kblocks - 1) + i
                if 0 <= j < kblocks:
                    for n in range(2):
                        total[p][2 * j + n] = (
                            total[p][2 * j + n]
                            + prod[i * SUBS : (i + 1) * SUBS, n * LANES : (n + 1) * LANES]
                        )
    for t in range(nspans):
        chunks[0, :, t * LANES : (t + 1) * LANES] = jnp.concatenate(
            [total[1][t], total[0][t]], axis=0
        ).astype(jnp.bfloat16)

    for d in (3, 1, 2):
        share(d).start()

    for d in range(1, PLANE):
        jplane(d).wait_recv()
    jnext(0).wait_recv()
    jprev(0).wait_recv()
    loads[2].wait()
    loads[3].wait()

    jit = msgs[0, SUBS : 2 * SUBS]
    for i in range(1, PLANE + 2):
        jit = jit + msgs[i, SUBS : 2 * SUBS]
    ahead = pltpu.roll(jit, LANES - 1, 1)
    behind = pltpu.roll(jit, 1, 1)
    weight = (1.0 + (ahead - behind) * 1.5) * (4.0 / math.sqrt(angles) / 65536)
    theta = ((lane % angles).astype(jnp.float32) + jit) * math.pi / angles
    cosine = jnp.cos(theta) * 0.5
    sine = jnp.sin(theta) * 0.5
    lead = sub % slices < slices // 2
    ypos = []
    for g in range(groups):
        row = ((sub % zper + g * zper) * PLANE + q) * rows_dev + sub // zper
        ypos.append(row.astype(jnp.float32) - (nrows - 1) / 2)

    def spread(d):
        inverse = 1.0 / msgs[d, :SUBS]
        words = []
        for t in range(nspans):
            both = chunks[d, :, t * LANES : (t + 1) * LANES].astype(jnp.float32)
            even = jnp.round(both[:SUBS] * inverse).astype(jnp.int32)
            odd = jnp.round(both[SUBS:] * inverse).astype(jnp.int32)
            high = jnp.where(lead, even, pltpu.roll(odd, 2, 0))
            low = jnp.where(lead, pltpu.roll(even, SUBS - 2, 0), odd)
            words.append(lax.shift_left(high, 16) + low)
            tab[4 * t + 1] = words[-1]
        for j in range(1, 4):
            cut = LANES - 32 * j
            turned = [pltpu.roll(word, cut, 1) for word in words]
            for t in range(nspans):
                after = turned[t + 1] if t + 1 < nspans else 0
                tab[4 * t + j + 1] = jnp.where(lane < cut, turned[t], after)
            if j == 3:
                tab[0] = jnp.where(lane < cut, 0, turned[0])

    def angle(d, i):
        first = peer(d) * ang_dev + i
        pick = jnp.full((SUBS, LANES), first, jnp.int32)
        cosb, sinb, wt = (lane_gather(x, pick) for x in (cosine, sine, weight))
        parts = [lanef * cosb + ypos[g] * sinb for g in range(groups)]
        scales = []
        for s in range(slices):
            line = jnp.broadcast_to(
                msgs[d, i * slices + s : i * slices + s + 1], (SUBS, LANES)
            )
            scales.append(line * wt)
        return cosb, parts, scales

    def line(slot, row):
        return jnp.broadcast_to(tab[slot, row : row + 1], (SUBS, LANES))

    def project(d, known, g, b):
        pc = peer(d)
        qc = pc - z * PLANE
        sums = [None] * slices
        for i in range(ang_dev):
            cosb, parts, scales = known[i]
            moved = shift_ref[pc * ang_dev + i]
            slot = base[0, ((qc * ang_dev + i) * nblocks + b) * groups + g]
            slot = lax.shift_right_arithmetic(slot + moved, 6)
            offset = (moved - slot * STEP).astype(jnp.float32) * 0.5 + (half + STEP) * 0.5
            h = cosb * (b * LANES - half) + parts[g] + offset
            odd = h.astype(jnp.int32)
            even = (h + 0.5).astype(jnp.int32)
            frac = jnp.abs(h - even.astype(jnp.float32)) * 2.0
            pairs = slices // 2
            evens = [lane_gather(line(slot, i * slices + s), even) for s in range(pairs)]
            odds = [lane_gather(line(slot, i * slices + pairs + s), odd) for s in range(pairs)]
            for s in range(slices):
                e, o = evens[s % pairs], odds[s % pairs]
                if s >= pairs:
                    e, o = lax.shift_left(e, 16), lax.shift_left(o, 16)
                e, o = e.astype(jnp.float32), o.astype(jnp.float32)
                got = (e + frac * (o - e)) * scales[s]
                sums[s] = got if sums[s] is None else sums[s] + got
        return sums

    spread(0)
    known = [angle(0, i) for i in range(ang_dev)]
    for b in range(nblocks):
        for g in range(groups):
            for s, val in enumerate(project(0, known, g, b)):
                acc[g, s, b] = val

    @pl.loop(1, PLANE - 1)
    def _(d):
        share(d).wait_recv()
        spread(d)
        known = [angle(d, i) for i in range(ang_dev)]
        for b in range(nblocks):
            for g in range(groups):
                for s, val in enumerate(project(d, known, g, b)):
                    acc[g, s, b] += val

    d = PLANE - 1
    share(d).wait_recv()
    spread(d)
    known = [angle(d, i) for i in range(ang_dev)]
    pos = sub % zper
    ntile = nblocks // 2 // PARTS
    for part in range(PARTS):
        for t in range(ntile):
            for g in range(groups):
                out = [[], [], [], []]
                for b in (2 * (part * ntile + t), 2 * (part * ntile + t) + 1):
                    v = [acc[g, s, b] + x for s, x in enumerate(project(d, known, g, b))]
                    w = [None] * 4
                    for s in range(2):
                        w[s] = jnp.where(pos < 2, v[s], pltpu.roll(v[s + 2], 2, 0))
                        w[s + 2] = jnp.where(pos < 2, pltpu.roll(v[s], SUBS - 2, 0), v[s + 2])
                    for s in (0, 2):
                        lo = jnp.where(pos % 2 < 1, w[s], pltpu.roll(w[s + 1], 1, 0))
                        hi = jnp.where(pos % 2 < 1, pltpu.roll(w[s], SUBS - 1, 0), w[s + 1])
                        for n, val in ((s, lo), (s + 1, hi)):
                            fin[g * zper + n, b] = val
                            out[n].append(val)
                for n in range(4):
                    snd[part, g * zper + n, :, t * LANES : (t + 1) * LANES] = jnp.concatenate(
                        out[n], axis=0
                    ).astype(jnp.bfloat16)

        @pl.loop(0, depth)
        def _(zt):
            @pl.when(zt != z)
            def _():
                give(zt, part).start()

    for part in range(PARTS):
        @pl.loop(1, depth)
        def _(k):
            take((z + k) % depth, part).wait_recv()

        for t in range(ntile):
            b = 2 * (part * ntile + t)
            sums = [fin[z, b], fin[z, b + 1]]
            for k in range(1, depth):
                both = rcv[part, (z + k) % depth, :, t * LANES : (t + 1) * LANES]
                both = both.astype(jnp.float32)
                sums = [sums[0] + both[:SUBS], sums[1] + both[SUBS:]]
            for j in range(2):
                cols = slice((b + j) * LANES, (b + j + 1) * LANES)
                for r in range(rows_dev):
                    out_ref[r, :, cols] = sums[j][r * slices : (r + 1) * slices]

    for d in range(1, PLANE):
        jplane(d).wait_send()
        share(d).wait_send()

    @pl.when(q == PLANE - 1)
    def _():
        for p in range(PLANE):
            jnext(p).wait_send()

    @pl.when(q == 0)
    def _():
        for p in range(PLANE):
            jprev(p).wait_send()

    for part in range(PARTS):
        @pl.loop(1, depth)
        def _(k):
            give((z + k) % depth, part).wait_send()


def body(sinogram, jitter, shift):
    width = lax.axis_size("blk")
    ang_dev, slices, bins = sinogram.shape
    angles = shift.shape[0]
    rows_dev = SUBS // slices
    depth = width // PLANE
    assert ang_dev == 2 and rows_dev == 2 and slices == 4 and LANES % angles == 0
    assert width % (PLANE * 4) == 0 and bins % (2 * BLOCK) == 0
    groups = depth * rows_dev // SUBS
    nblocks = bins // LANES
    anywhere = pl.BlockSpec(memory_space=pl.ANY)
    dma = pltpu.SemaphoreType.DMA
    slab = jnp.asarray(ramp_slab(bins))
    base = jnp.asarray(window_base(width, ang_dev, rows_dev, bins))
    return pl.pallas_call(
        functools.partial(kernel, width),
        out_shape=pltpu.VMEM((rows_dev, slices, bins), jnp.float32),
        in_specs=[anywhere] * 5,
        out_specs=pl.BlockSpec(memory_space=pltpu.VMEM),
        scratch_shapes=[
            pltpu.VMEM((1, ang_dev), jnp.bfloat16),
            pltpu.SMEM((angles,), jnp.int32),
            pltpu.VMEM((ang_dev, slices, bins), jnp.bfloat16),
            pltpu.VMEM(slab.shape, jnp.bfloat16),
            pltpu.SMEM(base.shape[1:], jnp.int32),
            pltpu.VMEM((PLANE, 2 * SUBS, bins // 2), jnp.bfloat16),
            pltpu.VMEM((PLANE + 2, 2 * SUBS, LANES), jnp.float32),
            pltpu.VMEM((bins // STEP + 2, SUBS, LANES), jnp.int32),
            pltpu.VMEM((groups, slices, nblocks, SUBS, LANES), jnp.float32),
            pltpu.VMEM((depth, nblocks, SUBS, LANES), jnp.float32),
            pltpu.VMEM((PARTS, depth, 2 * SUBS, bins // 2 // PARTS), jnp.bfloat16),
            pltpu.VMEM((PARTS, depth, 2 * SUBS, bins // 2 // PARTS), jnp.bfloat16),
            dma((4,)),
            dma((PIECES,)),
            dma((2 * PLANE - 1,)),
            dma((PLANE + 1,)),
            dma((PLANE - 1,)),
            dma((PLANE - 1,)),
            dma((PARTS, depth)),
            dma((PARTS, depth)),
        ],
        compiler_params=pltpu.CompilerParams(collective_id=0, has_side_effects=True),
    )(jitter.reshape(1, ang_dev), shift, sinogram, slab, base)


def solution(mesh):
    in_specs = (P("blk", "slab", None), P("blk"), P())
    out_specs = P("blk", "slab", None)
    return jax.shard_map(body, mesh=mesh, in_specs=in_specs, out_specs=out_specs, check_vma=False)
```

```python
import functools
import math

import jax
import jax.numpy as jnp
import numpy as np
from jax import lax
from jax.experimental import pallas as pl
from jax.experimental.pallas import tpu as pltpu
from jax.sharding import PartitionSpec as P

LANES = 128
SUBS = 8
BLOCK = 256
PLANE = 4
STEP = 64
JITTER = 0.29882812
SHIFT = 8
PIECES = 4
PARTS = 2
MESH = pl.DeviceIdType.MESH


def ramp_slab(bins):
    span = bins // 2
    first = -(span - LANES)
    offset = np.arange(first, span, dtype=np.int32)[None, :] - np.arange(LANES, dtype=np.int32)[:, None]
    both = 2 * np.stack([offset, offset - 1]) + 1
    safe = both.astype(np.float32)
    slab = (np.float32(-1.0) / (np.float32(math.pi**2) * safe * safe)).astype(jnp.bfloat16)
    tiles = slab.reshape(2, LANES, -1, LANES)
    return np.ascontiguousarray(tiles.transpose(2, 0, 1, 3))


def window_base(width, ang_dev, rows_dev, bins):
    depth = width // PLANE
    angles, nrows = width * ang_dev, width * rows_dev
    nblocks, per = bins // LANES, PLANE * ang_dev
    groups = depth * rows_dev // SUBS
    half = (bins - 1) / 2
    me = np.arange(width)
    z, q = me // PLANE, me % PLANE
    a = z[:, None] * per + np.arange(per)[None, :]
    theta = (a[..., None] + np.linspace(-JITTER, JITTER, 9)) * math.pi / angles
    zs = np.arange(groups)[:, None] * (SUBS // rows_dev) + np.array([0, SUBS // rows_dev - 1])
    rows = (zs[None] * PLANE + q[:, None, None]) * rows_dev + np.array([0, rows_dev - 1])
    y = rows - (nrows - 1) / 2
    x = np.arange(nblocks)[:, None] * LANES + np.array([0, LANES - 1]) - half
    u = (
        x[None, None, :, None, :, None, None] * np.cos(theta)[:, :, None, None, None, None, :]
        + y[:, None, None, :, None, :, None] * np.sin(theta)[:, :, None, None, None, None, :]
        + half
    )
    low = np.floor(u.min(axis=(4, 5, 6)) - 0.25).astype(np.int32)
    high = u.max(axis=(4, 5, 6)) + 0.25
    assert (high - low).max() + STEP < 2 * LANES
    assert low.min() - SHIFT >= -STEP and low.max() + SHIFT < bins + STEP
    return (low + STEP).reshape(width, 1, per * nblocks * groups)


def lane_gather(x, index):
    dims = lax.GatherDimensionNumbers(
        offset_dims=(),
        collapsed_slice_dims=(1,),
        start_index_map=(1,),
        operand_batching_dims=(0,),
        start_indices_batching_dims=(0,),
    )
    return lax.gather(
        x, index[..., None], dims, (1, 1), mode=lax.GatherScatterMode.PROMISE_IN_BOUNDS
    )


def kernel(
    width,
    jit_hbm,
    shift_hbm,
    sino_hbm,
    slab_hbm,
    base_hbm,
    out_ref,
    jit_ref,
    shift_ref,
    sino_ref,
    slab,
    base,
    chunks,
    msgs,
    tab,
    acc,
    own,
    wvec,
    fin,
    snd,
    rcv,
    lsem,
    wsem,
    sj,
    rj,
    s1,
    r1,
    s2,
    r2,
):
    me = lax.axis_index("blk")
    ang_dev, slices, bins = sino_ref.shape
    rows_dev = out_ref.shape[0]
    angles = width * ang_dev
    nrows = width * rows_dev
    nblocks = bins // LANES
    nspans = bins // BLOCK
    depth = width // PLANE
    groups = acc.shape[0]
    zper = SUBS // rows_dev
    z, q = me // PLANE, me % PLANE
    half = (bins - 1) / 2

    def remote(src, dst, send, recv, dev):
        return pltpu.make_async_remote_copy(
            src_ref=src,
            dst_ref=dst,
            send_sem=send,
            recv_sem=recv,
            device_id={"blk": dev},
            device_id_type=MESH,
        )

    loads = [
        pltpu.make_async_copy(src, dst, lsem.at[i])
        for i, (src, dst) in enumerate(
            [
                (jit_hbm, jit_ref),
                (sino_hbm, sino_ref),
                (shift_hbm, shift_ref),
                (base_hbm.at[me], base),
            ]
        )
    ]
    kblocks = bins // 2 // BLOCK
    ntiles = slab.shape[0]
    cuts = [0]
    for piece in range(PIECES):
        cuts.append(min(ntiles, 1 + 2 * -(-(2 * kblocks - 1) * (piece + 1) // PIECES)))
    weights = [
        pltpu.make_async_copy(
            slab_hbm.at[cuts[n] : cuts[n + 1]], slab.at[cuts[n] : cuts[n + 1]], wsem.at[n]
        )
        for n in range(PIECES)
    ]
    for load in loads[:2] + weights + loads[2:]:
        load.start()

    barrier = pltpu.get_barrier_semaphore()

    qx, qy = q % 2, q // 2
    ends = PLANE - 1

    def peer(d):
        return z * PLANE + (qx + d % 2) % 2 + 2 * ((qy + d // 2) % 2)

    def hello(dev):
        pl.semaphore_signal(barrier, inc=1, device_id={"blk": dev}, device_id_type=MESH)

    for d in (3, 1, 2):
        hello(peer(d))

    @pl.loop(1, depth)
    def _(k):
        hello((z + k) % depth * PLANE + q)

    @pl.when(q != ends)
    def _():
        hello((z + depth - 1) % depth * PLANE + ends)

    @pl.when((q != 0) & (z < depth - 1))
    def _():
        hello((z + 1) * PLANE)

    greeted = (
        ends + depth - 1
        + ends * (q // ends)
        + ends * ((PLANE - 1 - q) // ends) * ((z + depth - 1) // depth)
    )

    jrow = msgs.at[0, SUBS : 2 * SUBS]

    def jplane(d):
        return remote(msgs.at[0], msgs.at[d], sj.at[d - 1], rj.at[d - 1], peer(d))

    def jnext(p):
        return remote(
            jrow, msgs.at[PLANE, SUBS : 2 * SUBS], sj.at[PLANE - 1 + p], rj.at[PLANE - 1],
            (z + 1) % depth * PLANE + p,
        )

    def jprev(p):
        return remote(
            jrow, msgs.at[PLANE + 1, SUBS : 2 * SUBS], sj.at[PLANE - 1 + p], rj.at[PLANE],
            (z - 1) * PLANE + p,
        )

    def jwrap():
        return remote(
            msgs.at[q, SUBS : 2 * SUBS], msgs.at[PLANE + 1, SUBS : 2 * SUBS],
            sj.at[2 * PLANE - 1], rj.at[PLANE], (depth - 1) * PLANE + q,
        )

    def share(d):
        return remote(chunks.at[0], chunks.at[d], s1.at[d - 1], r1.at[d - 1], peer(d))

    def give(zt, part):
        return remote(
            snd.at[part, zt], rcv.at[part, z], s2.at[part, zt], r2.at[part, z], zt * PLANE + q
        )

    def take(zs, part):
        return remote(
            snd.at[part, zs], rcv.at[part, zs], s2.at[part, zs], r2.at[part, zs], zs * PLANE + q
        )

    lane = lax.broadcasted_iota(jnp.int32, (SUBS, LANES), 1)
    sub = lax.broadcasted_iota(jnp.int32, (SUBS, LANES), 0)
    lanef = lane.astype(jnp.float32)
    tab[tab.shape[0] - 1] = jnp.zeros((SUBS, LANES), jnp.int32)
    for g in range(groups):
        for s in range(slices):
            for b in range(nblocks):
                acc[g, s, b] = jnp.zeros((SUBS, LANES), jnp.float32)

    loads[0].wait()
    mine = (lane % angles) - me * ang_dev
    msg = jnp.zeros((SUBS, LANES), jnp.float32)
    for i in range(ang_dev):
        msg = jnp.where(mine == i, jit_ref[0:1, i : i + 1].astype(jnp.float32), msg)
    msgs[0, SUBS : 2 * SUBS] = msg

    loads[1].wait()
    flat = jnp.concatenate(
        [sino_ref[i].astype(jnp.float32) for i in range(ang_dev)], axis=0
    )
    tiles = [flat[:, b * LANES : (b + 1) * LANES] for b in range(nblocks)]
    top = jnp.abs(tiles[0])
    for tile in tiles[1:]:
        top = jnp.maximum(top, jnp.abs(tile))
    top = jnp.broadcast_to(jnp.max(top, axis=1, keepdims=True), (SUBS, LANES))
    msgs[0, :SUBS] = jnp.maximum(top, 1e-30) * (0.51 / 32700)

    pl.semaphore_wait(barrier, greeted)

    for d in (3, 1, 2):
        jplane(d).start()

    @pl.when(q == PLANE - 1)
    def _():
        for p in range(PLANE):
            jnext(p).start()

    @pl.when((q == 0) & (z > 0))
    def _():
        for p in range(PLANE):
            jprev(p).start()

    @pl.when((q == 0) & (z == 0))
    def _():
        jwrap().start()

    split = []
    for p in range(2):
        index = (2 * lane + p) % LANES
        picked = [lane_gather(tile, index) for tile in tiles]
        split.append(
            [
                jnp.where(lane < LANES // 2, picked[2 * t], picked[2 * t + 1])
                for t in range(nspans)
            ]
        )
    lhs = [
        jnp.concatenate(
            [jnp.concatenate([part[2 * k], part[2 * k + 1]], axis=1) for k in range(kblocks)],
            axis=0,
        ).astype(jnp.bfloat16)
        for part in split
    ]
    total = [
        [split[1 - p][t] * 0.25 for t in range(nspans)] for p in range(2)
    ]
    ready = 0
    for d in range(2 * kblocks - 1):
        while cuts[ready] < 2 * d + 3:
            weights[ready].wait()
            ready += 1
        for p in range(2):
            up = jnp.concatenate([slab[2 * d + 1, p], slab[2 * d + 2, p]], axis=1)
            down = jnp.concatenate([slab[2 * d, p], slab[2 * d + 1, p]], axis=1)
            prod = jnp.dot(
                lhs[p], jnp.concatenate([up, down], axis=0), preferred_element_type=jnp.float32
            )
            for i in range(kblocks):
                j = d - (kblocks - 1) + i
                if 0 <= j < kblocks:
                    for n in range(2):
                        total[p][2 * j + n] = (
                            total[p][2 * j + n]
                            + prod[i * SUBS : (i + 1) * SUBS, n * LANES : (n + 1) * LANES]
                        )
    for t in range(nspans):
        chunks[0, :, t * LANES : (t + 1) * LANES] = jnp.concatenate(
            [total[1][t], total[0][t]], axis=0
        ).astype(jnp.bfloat16)

    for d in (3, 1, 2):
        share(d).start()

    loads[2].wait()
    loads[3].wait()

    def waves(jit):
        theta = ((lane % angles).astype(jnp.float32) + jit) * math.pi / angles
        return jnp.cos(theta) * 0.5, jnp.sin(theta) * 0.5

    def weigh(jit):
        ahead = pltpu.roll(jit, LANES - 1, 1)
        behind = pltpu.roll(jit, 1, 1)
        return (1.0 + (ahead - behind) * 1.5) * (4.0 / math.sqrt(angles))

    lead = sub % slices < slices // 2
    ypos = []
    for g in range(groups):
        row = ((sub % zper + g * zper) * PLANE + q) * rows_dev + sub // zper
        ypos.append(row.astype(jnp.float32) - (nrows - 1) / 2)

    def spread(d):
        inverse = 1.0 / msgs[d, :SUBS]
        words = []
        for t in range(nspans):
            both = chunks[d, :, t * LANES : (t + 1) * LANES].astype(jnp.float32)
            even = jnp.round(both[:SUBS] * inverse).astype(jnp.int32)
            odd = jnp.round(both[SUBS:] * inverse).astype(jnp.int32)
            high = jnp.where(lead, even, pltpu.roll(odd, 2, 0))
            low = jnp.where(lead, pltpu.roll(even, SUBS - 2, 0), odd)
            words.append(lax.shift_left(high, 16) + low)
            tab[4 * t + 1] = words[-1]
        for j in range(1, 4):
            cut = LANES - 32 * j
            turned = [pltpu.roll(word, cut, 1) for word in words]
            for t in range(nspans):
                after = turned[t + 1] if t + 1 < nspans else 0
                tab[4 * t + j + 1] = jnp.where(lane < cut, turned[t], after)
            if j == 3:
                tab[0] = jnp.where(lane < cut, 0, turned[0])

    def angle(d, i, wave, weight):
        pick = jnp.full((SUBS, LANES), peer(d) * ang_dev + i, jnp.int32)
        cosb, sinb = (lane_gather(x, pick) for x in wave)
        parts = [lanef * cosb + ypos[g] * sinb for g in range(groups)]
        wt = 1.0 if weight is None else lane_gather(weight, pick)
        scales = []
        for s in range(slices):
            row = i * slices + s
            scale = jnp.broadcast_to(msgs[d, row : row + 1], (SUBS, LANES))
            scales.append(scale * (wt * (1.0 / 65536)))
        return cosb, parts, scales

    def line(slot, row):
        return jnp.broadcast_to(tab[slot, row : row + 1], (SUBS, LANES))

    def project(d, known, g, b):
        pc = peer(d)
        qc = pc - z * PLANE
        sums = []
        for i in range(ang_dev):
            cosb, parts, scales = known[i]
            moved = shift_ref[pc * ang_dev + i]
            slot = base[0, ((qc * ang_dev + i) * nblocks + b) * groups + g]
            slot = lax.shift_right_arithmetic(slot + moved, 6)
            offset = (moved - slot * STEP).astype(jnp.float32) * 0.5 + (half + STEP) * 0.5
            h = cosb * (b * LANES - half) + parts[g] + offset
            odd = h.astype(jnp.int32)
            even = (h + 0.5).astype(jnp.int32)
            frac = jnp.abs(h - even.astype(jnp.float32)) * 2.0
            pairs = slices // 2
            evens = [lane_gather(line(slot, i * slices + s), even) for s in range(pairs)]
            odds = [lane_gather(line(slot, i * slices + pairs + s), odd) for s in range(pairs)]
            got = []
            for s in range(slices):
                e, o = evens[s % pairs], odds[s % pairs]
                if s >= pairs:
                    e, o = lax.shift_left(e, 16), lax.shift_left(o, 16)
                e, o = e.astype(jnp.float32), o.astype(jnp.float32)
                got.append((e + frac * (o - e)) * scales[s])
            sums.append(got)
        return sums

    spread(0)
    wave = waves(msgs[0, SUBS : 2 * SUBS])
    known = [angle(0, i, wave, None) for i in range(ang_dev)]
    for b in range(nblocks):
        for g in range(groups):
            for i, got in enumerate(project(0, known, g, b)):
                for s in range(slices):
                    own[i, g, s, b] = got[s]

    for d in range(1, PLANE):
        jplane(d).wait_recv()

    @pl.when((q > 0) & (z == 0))
    def _():
        jwrap().start()

    def known_jitter(slots):
        jit = msgs[0, SUBS : 2 * SUBS]
        for i in range(1, slots):
            jit = jit + msgs[i, SUBS : 2 * SUBS]
        return jit

    for i, x in enumerate(waves(known_jitter(PLANE))):
        wvec[i] = x
    wvec[2] = weigh(known_jitter(PLANE))

    order = [1 + 2 * ((qx + qy) % 2), 2 - qx * (1 - qy)]
    order.append(6 - order[0] - order[1])

    @pl.loop(0, PLANE - 2)
    def _(step):
        @pl.when(step == 1)
        def _():
            jnext(0).wait_recv()
            wvec[2] = weigh(known_jitter(PLANE + 1))

        d = order[0] + step * (order[1] - order[0])
        share(d).wait_recv()
        spread(d)
        known = [angle(d, i, (wvec[0], wvec[1]), wvec[2]) for i in range(ang_dev)]
        for b in range(nblocks):
            for g in range(groups):
                first, second = project(d, known, g, b)
                for s in range(slices):
                    acc[g, s, b] += first[s] + second[s]

    d = order[2]
    jprev(0).wait_recv()
    share(d).wait_recv()
    weight = weigh(known_jitter(PLANE + 2))
    spread(d)
    known = [angle(d, i, (wvec[0], wvec[1]), weight) for i in range(ang_dev)]
    mine = [
        lane_gather(weight, jnp.full((SUBS, LANES), me * ang_dev + i, jnp.int32))
        for i in range(ang_dev)
    ]
    pos = sub % zper
    ntile = nblocks // 2 // PARTS
    for part in range(PARTS):
        for t in range(ntile):
            for g in range(groups):
                out = [[], [], [], []]
                for b in (2 * (part * ntile + t), 2 * (part * ntile + t) + 1):
                    first, second = project(d, known, g, b)
                    v = [
                        (acc[g, s, b] + mine[0] * own[0, g, s, b])
                        + (mine[1] * own[1, g, s, b] + (first[s] + second[s]))
                        for s in range(slices)
                    ]
                    w = [None] * 4
                    for s in range(2):
                        w[s] = jnp.where(pos < 2, v[s], pltpu.roll(v[s + 2], 2, 0))
                        w[s + 2] = jnp.where(pos < 2, pltpu.roll(v[s], SUBS - 2, 0), v[s + 2])
                    for s in (0, 2):
                        lo = jnp.where(pos % 2 < 1, w[s], pltpu.roll(w[s + 1], 1, 0))
                        hi = jnp.where(pos % 2 < 1, pltpu.roll(w[s], SUBS - 1, 0), w[s + 1])
                        for n, val in ((s, lo), (s + 1, hi)):
                            fin[g * zper + n, b] = val
                            out[n].append(val)
                for n in range(4):
                    snd[part, g * zper + n, :, t * LANES : (t + 1) * LANES] = jnp.concatenate(
                        out[n], axis=0
                    ).astype(jnp.bfloat16)

        @pl.loop(0, depth)
        def _(zt):
            @pl.when(zt != z)
            def _():
                give(zt, part).start()

    for part in range(PARTS):
        @pl.loop(1, depth)
        def _(k):
            take((z + k) % depth, part).wait_recv()

        for t in range(ntile):
            b = 2 * (part * ntile + t)
            sums = [fin[z, b], fin[z, b + 1]]
            for k in range(1, depth):
                both = rcv[part, (z + k) % depth, :, t * LANES : (t + 1) * LANES]
                both = both.astype(jnp.float32)
                sums = [sums[0] + both[:SUBS], sums[1] + both[SUBS:]]
            for j in range(2):
                cols = slice((b + j) * LANES, (b + j + 1) * LANES)
                for r in range(rows_dev):
                    out_ref[r, :, cols] = sums[j][r * slices : (r + 1) * slices]

    for d in range(1, PLANE):
        jplane(d).wait_send()
        share(d).wait_send()

    @pl.when(q == PLANE - 1)
    def _():
        for p in range(PLANE):
            jnext(p).wait_send()

    @pl.when((q == 0) & (z > 0))
    def _():
        for p in range(PLANE):
            jprev(p).wait_send()

    @pl.when(z == 0)
    def _():
        jwrap().wait_send()

    for part in range(PARTS):
        @pl.loop(1, depth)
        def _(k):
            give((z + k) % depth, part).wait_send()


def body(sinogram, jitter, shift):
    width = lax.axis_size("blk")
    ang_dev, slices, bins = sinogram.shape
    angles = shift.shape[0]
    rows_dev = SUBS // slices
    depth = width // PLANE
    assert ang_dev == 2 and rows_dev == 2 and slices == 4 and LANES % angles == 0
    assert width % (PLANE * 4) == 0 and bins % (2 * BLOCK) == 0
    groups = depth * rows_dev // SUBS
    nblocks = bins // LANES
    anywhere = pl.BlockSpec(memory_space=pl.ANY)
    dma = pltpu.SemaphoreType.DMA
    slab = jnp.asarray(ramp_slab(bins))
    base = jnp.asarray(window_base(width, ang_dev, rows_dev, bins))
    return pl.pallas_call(
        functools.partial(kernel, width),
        out_shape=pltpu.VMEM((rows_dev, slices, bins), jnp.float32),
        in_specs=[anywhere] * 5,
        out_specs=pl.BlockSpec(memory_space=pltpu.VMEM),
        scratch_shapes=[
            pltpu.VMEM((1, ang_dev), jnp.bfloat16),
            pltpu.SMEM((angles,), jnp.int32),
            pltpu.VMEM((ang_dev, slices, bins), jnp.bfloat16),
            pltpu.VMEM(slab.shape, jnp.bfloat16),
            pltpu.SMEM(base.shape[1:], jnp.int32),
            pltpu.VMEM((PLANE, 2 * SUBS, bins // 2), jnp.bfloat16),
            pltpu.VMEM((PLANE + 2, 2 * SUBS, LANES), jnp.float32),
            pltpu.VMEM((bins // STEP + 2, SUBS, LANES), jnp.int32),
            pltpu.VMEM((groups, slices, nblocks, SUBS, LANES), jnp.float32),
            pltpu.VMEM((ang_dev, groups, slices, nblocks, SUBS, LANES), jnp.float32),
            pltpu.VMEM((3, SUBS, LANES), jnp.float32),
            pltpu.VMEM((depth, nblocks, SUBS, LANES), jnp.float32),
            pltpu.VMEM((PARTS, depth, 2 * SUBS, bins // 2 // PARTS), jnp.bfloat16),
            pltpu.VMEM((PARTS, depth, 2 * SUBS, bins // 2 // PARTS), jnp.bfloat16),
            dma((4,)),
            dma((PIECES,)),
            dma((2 * PLANE,)),
            dma((PLANE + 1,)),
            dma((PLANE - 1,)),
            dma((PLANE - 1,)),
            dma((PARTS, depth)),
            dma((PARTS, depth)),
        ],
        compiler_params=pltpu.CompilerParams(collective_id=0, has_side_effects=True),
    )(jitter.reshape(1, ang_dev), shift, sinogram, slab, base)


def solution(mesh):
    in_specs = (P("blk", "slab", None), P("blk"), P())
    out_specs = P("blk", "slab", None)
    return jax.shard_map(body, mesh=mesh, in_specs=in_specs, out_specs=out_specs, check_vma=False)
```

```python
import functools
import math

import jax
import jax.numpy as jnp
import numpy as np
from jax import lax
from jax.experimental import pallas as pl
from jax.experimental.pallas import tpu as pltpu
from jax.sharding import PartitionSpec as P

LANES = 128
SUBS = 8
BLOCK = 256
PLANE = 4
STEP = 64
JITTER = 0.29882812
SHIFT = 8
PIECES = 2
PARTS = 1
SENDS = (3, 1, 2)
MESH = pl.DeviceIdType.MESH


def ramp_slab(bins):
    span = bins // 2
    first = -(span - LANES)
    offset = np.arange(first, span, dtype=np.int32)[None, :] - np.arange(LANES, dtype=np.int32)[:, None]
    both = 2 * np.stack([offset, offset - 1]) + 1
    safe = both.astype(np.float32)
    slab = (np.float32(-1.0) / (np.float32(math.pi**2) * safe * safe)).astype(jnp.bfloat16)
    tiles = slab.reshape(2, LANES, -1, LANES)
    return np.ascontiguousarray(tiles.transpose(2, 0, 1, 3))


def window_base(width, ang_dev, rows_dev, bins):
    depth = width // PLANE
    angles, nrows = width * ang_dev, width * rows_dev
    nblocks, per = bins // LANES, PLANE * ang_dev
    groups = depth * rows_dev // SUBS
    half = (bins - 1) / 2
    me = np.arange(width)
    z, q = me // PLANE, me % PLANE
    a = z[:, None] * per + np.arange(per)[None, :]
    theta = (a[..., None] + np.linspace(-JITTER, JITTER, 9)) * math.pi / angles
    zs = np.arange(groups)[:, None] * (SUBS // rows_dev) + np.array([0, SUBS // rows_dev - 1])
    rows = (zs[None] * PLANE + q[:, None, None]) * rows_dev + np.array([0, rows_dev - 1])
    y = rows - (nrows - 1) / 2
    x = np.arange(nblocks)[:, None] * LANES + np.array([0, LANES - 1]) - half
    u = (
        x[None, None, :, None, :, None, None] * np.cos(theta)[:, :, None, None, None, None, :]
        + y[:, None, None, :, None, :, None] * np.sin(theta)[:, :, None, None, None, None, :]
        + half
    )
    low = np.floor(u.min(axis=(4, 5, 6)) - 0.25).astype(np.int32)
    high = u.max(axis=(4, 5, 6)) + 0.25
    assert (high - low).max() + STEP < 2 * LANES
    assert low.min() - SHIFT >= -STEP and low.max() + SHIFT < bins + STEP
    return (low + STEP).reshape(width, 1, per * nblocks * groups)


def lane_gather(x, index):
    dims = lax.GatherDimensionNumbers(
        offset_dims=(),
        collapsed_slice_dims=(1,),
        start_index_map=(1,),
        operand_batching_dims=(0,),
        start_indices_batching_dims=(0,),
    )
    return lax.gather(
        x, index[..., None], dims, (1, 1), mode=lax.GatherScatterMode.PROMISE_IN_BOUNDS
    )


def kernel(
    width,
    jit_hbm,
    shift_hbm,
    sino_hbm,
    slab_hbm,
    base_hbm,
    out_ref,
    jit_ref,
    shift_ref,
    sino_ref,
    slab,
    base,
    chunks,
    msgs,
    tab,
    held,
    fin,
    snd,
    rcv,
    lsem,
    wsem,
    sj,
    rj,
    s1,
    r1,
    s2,
    r2,
):
    me = lax.axis_index("blk")
    ang_dev, slices, bins = sino_ref.shape
    rows_dev = out_ref.shape[0]
    angles = width * ang_dev
    nrows = width * rows_dev
    nblocks = bins // LANES
    nspans = bins // BLOCK
    depth = width // PLANE
    groups = held.shape[2]
    zper = SUBS // rows_dev
    z, q = me // PLANE, me % PLANE
    half = (bins - 1) / 2

    def remote(src, dst, send, recv, dev):
        return pltpu.make_async_remote_copy(
            src_ref=src,
            dst_ref=dst,
            send_sem=send,
            recv_sem=recv,
            device_id={"blk": dev},
            device_id_type=MESH,
        )

    loads = [
        pltpu.make_async_copy(src, dst, lsem.at[i])
        for i, (src, dst) in enumerate(
            [
                (jit_hbm, jit_ref),
                (sino_hbm, sino_ref),
                (shift_hbm, shift_ref),
                (base_hbm.at[me], base),
            ]
        )
    ]
    kblocks = bins // 2 // BLOCK
    ntiles = slab.shape[0]
    cuts = [0]
    for piece in range(PIECES):
        cuts.append(min(ntiles, 1 + 2 * -(-(2 * kblocks - 1) * (piece + 1) // PIECES)))
    weights = [
        pltpu.make_async_copy(
            slab_hbm.at[cuts[n] : cuts[n + 1]], slab.at[cuts[n] : cuts[n + 1]], wsem.at[n]
        )
        for n in range(PIECES)
    ]
    for load in loads[:2] + weights + loads[2:]:
        load.start()

    barrier = pltpu.get_barrier_semaphore()

    qx, qy = q % 2, q // 2
    ends = PLANE - 1

    def peer(d):
        return z * PLANE + (qx + d % 2) % 2 + 2 * ((qy + d // 2) % 2)

    def hello(dev):
        pl.semaphore_signal(barrier, inc=1, device_id={"blk": dev}, device_id_type=MESH)

    for d in (3, 1, 2):
        hello(peer(d))

    @pl.loop(1, depth)
    def _(k):
        hello((z + k) % depth * PLANE + q)

    @pl.when(q != ends)
    def _():
        hello((z + depth - 1) % depth * PLANE + ends)

    @pl.when((q != 0) & (z < depth - 1))
    def _():
        hello((z + 1) * PLANE)

    greeted = (
        ends + depth - 1
        + ends * (q // ends)
        + ends * ((PLANE - 1 - q) // ends) * ((z + depth - 1) // depth)
    )

    jrow = msgs.at[0, SUBS : 2 * SUBS]

    def jplane(d):
        return remote(msgs.at[0], msgs.at[d], sj.at[d - 1], rj.at[d - 1], peer(d))

    def jnext(p):
        return remote(
            jrow, msgs.at[PLANE, SUBS : 2 * SUBS], sj.at[PLANE - 1 + p], rj.at[PLANE - 1],
            (z + 1) % depth * PLANE + p,
        )

    def jprev(p):
        return remote(
            jrow, msgs.at[PLANE + 1, SUBS : 2 * SUBS], sj.at[PLANE - 1 + p], rj.at[PLANE],
            (z - 1) * PLANE + p,
        )

    def jwrap():
        return remote(
            msgs.at[q, SUBS : 2 * SUBS], msgs.at[PLANE + 1, SUBS : 2 * SUBS],
            sj.at[2 * PLANE - 1], rj.at[PLANE], (depth - 1) * PLANE + q,
        )

    def share(d):
        return remote(chunks.at[0], chunks.at[d], s1.at[d - 1], r1.at[d - 1], peer(d))

    def give(zt, part):
        return remote(
            snd.at[part, zt], rcv.at[part, z], s2.at[part, zt], r2.at[part, z], zt * PLANE + q
        )

    def take(zs, part):
        return remote(
            snd.at[part, zs], rcv.at[part, zs], s2.at[part, zs], r2.at[part, zs], zs * PLANE + q
        )

    lane = lax.broadcasted_iota(jnp.int32, (SUBS, LANES), 1)
    sub = lax.broadcasted_iota(jnp.int32, (SUBS, LANES), 0)
    lanef = lane.astype(jnp.float32)
    tab[tab.shape[0] - 1] = jnp.zeros((SUBS, LANES), jnp.int32)

    loads[0].wait()
    mine = (lane % angles) - me * ang_dev
    msg = jnp.zeros((SUBS, LANES), jnp.float32)
    for i in range(ang_dev):
        msg = jnp.where(mine == i, jit_ref[0:1, i : i + 1].astype(jnp.float32), msg)
    theta = ((lane % angles).astype(jnp.float32) + msg) * math.pi / angles
    waves = [jnp.cos(theta) * 0.5, jnp.sin(theta) * 0.5]
    body = msg
    for i in range(ang_dev):
        pick = jnp.full((SUBS, LANES), me * ang_dev + i, jnp.int32)
        for n in range(2):
            body = jnp.where(sub == 1 + 2 * i + n, lane_gather(waves[n], pick), body)
    msgs[0, SUBS : 2 * SUBS] = body

    loads[1].wait()
    flat = jnp.concatenate(
        [sino_ref[i].astype(jnp.float32) for i in range(ang_dev)], axis=0
    )
    tiles = [flat[:, b * LANES : (b + 1) * LANES] for b in range(nblocks)]
    top = jnp.abs(tiles[0])
    for tile in tiles[1:]:
        top = jnp.maximum(top, jnp.abs(tile))
    top = jnp.broadcast_to(jnp.max(top, axis=1, keepdims=True), (SUBS, LANES))
    msgs[0, :SUBS] = jnp.maximum(top, 1e-30) * (0.51 / 32700)

    split = []
    for p in range(2):
        index = (2 * lane + p) % LANES
        picked = [lane_gather(tile, index) for tile in tiles]
        split.append(
            [
                jnp.where(lane < LANES // 2, picked[2 * t], picked[2 * t + 1])
                for t in range(nspans)
            ]
        )
    lhs = [
        jnp.concatenate(
            [jnp.concatenate([part[2 * k], part[2 * k + 1]], axis=1) for k in range(kblocks)],
            axis=0,
        ).astype(jnp.bfloat16)
        for part in split
    ]
    total = [
        [split[1 - p][t] * 0.25 for t in range(nspans)] for p in range(2)
    ]
    ready = 0
    for d in range(2 * kblocks - 1):
        while cuts[ready] < 2 * d + 3:
            weights[ready].wait()
            ready += 1
        for p in range(2):
            up = jnp.concatenate([slab[2 * d + 1, p], slab[2 * d + 2, p]], axis=1)
            down = jnp.concatenate([slab[2 * d, p], slab[2 * d + 1, p]], axis=1)
            prod = jnp.dot(
                lhs[p], jnp.concatenate([up, down], axis=0), preferred_element_type=jnp.float32
            )
            for i in range(kblocks):
                j = d - (kblocks - 1) + i
                if 0 <= j < kblocks:
                    for n in range(2):
                        total[p][2 * j + n] = (
                            total[p][2 * j + n]
                            + prod[i * SUBS : (i + 1) * SUBS, n * LANES : (n + 1) * LANES]
                        )
    for t in range(nspans):
        chunks[0, :, t * LANES : (t + 1) * LANES] = jnp.concatenate(
            [total[1][t], total[0][t]], axis=0
        ).astype(jnp.bfloat16)

    pl.semaphore_wait(barrier, greeted)

    for d in (3, 1, 2):
        jplane(d).start()

    @pl.when(q == PLANE - 1)
    def _():
        for p in range(PLANE):
            jnext(p).start()

    @pl.when((q == 0) & (z > 0))
    def _():
        for p in range(PLANE):
            jprev(p).start()

    @pl.when((q == 0) & (z == 0))
    def _():
        jwrap().start()

    for d in SENDS:
        share(d).start()

    loads[2].wait()
    loads[3].wait()

    lead = sub % slices < slices // 2
    ypos = []
    for g in range(groups):
        row = ((sub % zper + g * zper) * PLANE + q) * rows_dev + sub // zper
        ypos.append(row.astype(jnp.float32) - (nrows - 1) / 2)

    def spread(d):
        inverse = 1.0 / msgs[d, :SUBS]
        words = []
        for t in range(nspans):
            both = chunks[d, :, t * LANES : (t + 1) * LANES].astype(jnp.float32)
            even = jnp.round(both[:SUBS] * inverse).astype(jnp.int32)
            odd = jnp.round(both[SUBS:] * inverse).astype(jnp.int32)
            high = jnp.where(lead, even, pltpu.roll(odd, 2, 0))
            low = jnp.where(lead, pltpu.roll(even, SUBS - 2, 0), odd)
            words.append(lax.shift_left(high, 16) + low)
            tab[4 * t + 1] = words[-1]
        for j in range(1, 4):
            cut = LANES - 32 * j
            turned = [pltpu.roll(word, cut, 1) for word in words]
            for t in range(nspans):
                after = turned[t + 1] if t + 1 < nspans else 0
                tab[4 * t + j + 1] = jnp.where(lane < cut, turned[t], after)
            if j == 3:
                tab[0] = jnp.where(lane < cut, 0, turned[0])

    def spoken(d, row):
        return jnp.broadcast_to(msgs[d, row : row + 1], (SUBS, LANES))

    def angle(d, i):
        cosb, sinb = (spoken(d, SUBS + 1 + 2 * i + n) for n in range(2))
        parts = [lanef * cosb + ypos[g] * sinb for g in range(groups)]
        scales = [spoken(d, i * slices + s) * (1.0 / 65536) for s in range(slices)]
        return cosb, parts, scales

    def line(slot, row):
        return jnp.broadcast_to(tab[slot, row : row + 1], (SUBS, LANES))

    def project(d, known, g, b):
        pc = peer(d)
        qc = pc - z * PLANE
        sums = []
        for i in range(ang_dev):
            cosb, parts, scales = known[i]
            moved = shift_ref[pc * ang_dev + i]
            slot = base[0, ((qc * ang_dev + i) * nblocks + b) * groups + g]
            slot = lax.shift_right_arithmetic(slot + moved, 6)
            offset = (moved - slot * STEP).astype(jnp.float32) * 0.5 + (half + STEP) * 0.5
            h = cosb * (b * LANES - half) + parts[g] + offset
            odd = h.astype(jnp.int32)
            even = (h + 0.5).astype(jnp.int32)
            frac = jnp.abs(h - even.astype(jnp.float32)) * 2.0
            pairs = slices // 2
            evens = [lane_gather(line(slot, i * slices + s), even) for s in range(pairs)]
            odds = [lane_gather(line(slot, i * slices + pairs + s), odd) for s in range(pairs)]
            got = []
            for s in range(slices):
                e, o = evens[s % pairs], odds[s % pairs]
                if s >= pairs:
                    e, o = lax.shift_left(e, 16), lax.shift_left(o, 16)
                e, o = e.astype(jnp.float32), o.astype(jnp.float32)
                got.append((e + frac * (o - e)) * scales[s])
            sums.append(got)
        return sums

    def keep(d):
        spread(d)
        known = [angle(d, i) for i in range(ang_dev)]
        for b in range(nblocks):
            for g in range(groups):
                for i, got in enumerate(project(d, known, g, b)):
                    for s in range(slices):
                        held[d, i, g, s, b] = got[s]

    keep(0)

    @pl.when((q > 0) & (z == 0))
    def _():
        jplane(q).wait_recv()
        jwrap().start()

    @pl.loop(1, PLANE - 1)
    def _(d):
        @pl.when((z > 0) | (q != d))
        def _():
            jplane(d).wait_recv()

        share(d).wait_recv()
        keep(d)

    d = PLANE - 1

    @pl.when((z > 0) | (q != d))
    def _():
        jplane(d).wait_recv()

    jnext(0).wait_recv()
    jprev(0).wait_recv()
    share(d).wait_recv()
    jit = sum(spoken(i, SUBS) for i in range(PLANE + 2))
    ahead = pltpu.roll(jit, LANES - 1, 1)
    behind = pltpu.roll(jit, 1, 1)
    weight = (1.0 + (ahead - behind) * 1.5) * (4.0 / math.sqrt(angles))
    weight = [
        [
            lane_gather(weight, jnp.full((SUBS, LANES), peer(n) * ang_dev + i, jnp.int32))
            for i in range(ang_dev)
        ]
        for n in range(PLANE)
    ]
    spread(d)
    known = [angle(d, i) for i in range(ang_dev)]
    pos = sub % zper
    ntile = nblocks // 2 // PARTS
    for part in range(PARTS):
        for t in range(ntile):
            for g in range(groups):
                out = [[], [], [], []]
                for b in (2 * (part * ntile + t), 2 * (part * ntile + t) + 1):
                    got = project(d, known, g, b)
                    v = []
                    for s in range(slices):
                        terms = [weight[d][i] * got[i][s] for i in range(ang_dev)]
                        for n in range(PLANE - 1):
                            terms += [weight[n][i] * held[n, i, g, s, b] for i in range(ang_dev)]
                        while len(terms) > 1:
                            terms = [x + y for x, y in zip(terms[::2], terms[1::2])]
                        v += terms
                    w = [None] * 4
                    for s in range(2):
                        w[s] = jnp.where(pos < 2, v[s], pltpu.roll(v[s + 2], 2, 0))
                        w[s + 2] = jnp.where(pos < 2, pltpu.roll(v[s], SUBS - 2, 0), v[s + 2])
                    for s in (0, 2):
                        lo = jnp.where(pos % 2 < 1, w[s], pltpu.roll(w[s + 1], 1, 0))
                        hi = jnp.where(pos % 2 < 1, pltpu.roll(w[s], SUBS - 1, 0), w[s + 1])
                        for n, val in ((s, lo), (s + 1, hi)):
                            fin[g * zper + n, b] = val
                            out[n].append(val)
                for n in range(4):
                    snd[part, g * zper + n, :, t * LANES : (t + 1) * LANES] = jnp.concatenate(
                        out[n], axis=0
                    ).astype(jnp.bfloat16)

        @pl.loop(0, depth)
        def _(zt):
            @pl.when(zt != z)
            def _():
                give(zt, part).start()

    for part in range(PARTS):
        @pl.loop(1, depth)
        def _(k):
            take((z + k) % depth, part).wait_recv()

        for t in range(ntile):
            b = 2 * (part * ntile + t)
            sums = [fin[z, b], fin[z, b + 1]]
            for k in range(1, depth):
                both = rcv[part, (z + k) % depth, :, t * LANES : (t + 1) * LANES]
                both = both.astype(jnp.float32)
                sums = [sums[0] + both[:SUBS], sums[1] + both[SUBS:]]
            for j in range(2):
                cols = slice((b + j) * LANES, (b + j + 1) * LANES)
                for r in range(rows_dev):
                    out_ref[r, :, cols] = sums[j][r * slices : (r + 1) * slices]

    for d in range(1, PLANE):
        jplane(d).wait_send()
        share(d).wait_send()

    @pl.when(q == PLANE - 1)
    def _():
        for p in range(PLANE):
            jnext(p).wait_send()

    @pl.when((q == 0) & (z > 0))
    def _():
        for p in range(PLANE):
            jprev(p).wait_send()

    @pl.when(z == 0)
    def _():
        jwrap().wait_send()

    for part in range(PARTS):
        @pl.loop(1, depth)
        def _(k):
            give((z + k) % depth, part).wait_send()


def body(sinogram, jitter, shift):
    width = lax.axis_size("blk")
    ang_dev, slices, bins = sinogram.shape
    angles = shift.shape[0]
    rows_dev = SUBS // slices
    depth = width // PLANE
    assert ang_dev == 2 and rows_dev == 2 and slices == 4 and LANES % angles == 0
    assert width % (PLANE * 4) == 0 and bins % (2 * BLOCK) == 0
    groups = depth * rows_dev // SUBS
    nblocks = bins // LANES
    anywhere = pl.BlockSpec(memory_space=pl.ANY)
    dma = pltpu.SemaphoreType.DMA
    slab = jnp.asarray(ramp_slab(bins))
    base = jnp.asarray(window_base(width, ang_dev, rows_dev, bins))
    return pl.pallas_call(
        functools.partial(kernel, width),
        out_shape=pltpu.VMEM((rows_dev, slices, bins), jnp.float32),
        in_specs=[anywhere] * 5,
        out_specs=pl.BlockSpec(memory_space=pltpu.VMEM),
        scratch_shapes=[
            pltpu.VMEM((1, ang_dev), jnp.bfloat16),
            pltpu.SMEM((angles,), jnp.int32),
            pltpu.VMEM((ang_dev, slices, bins), jnp.bfloat16),
            pltpu.VMEM(slab.shape, jnp.bfloat16),
            pltpu.SMEM(base.shape[1:], jnp.int32),
            pltpu.VMEM((PLANE, 2 * SUBS, bins // 2), jnp.bfloat16),
            pltpu.VMEM((PLANE + 2, 2 * SUBS, LANES), jnp.float32),
            pltpu.VMEM((bins // STEP + 2, SUBS, LANES), jnp.int32),
            pltpu.VMEM((PLANE - 1, ang_dev, groups, slices, nblocks, SUBS, LANES), jnp.float32),
            pltpu.VMEM((depth, nblocks, SUBS, LANES), jnp.float32),
            pltpu.VMEM((PARTS, depth, 2 * SUBS, bins // 2 // PARTS), jnp.bfloat16),
            pltpu.VMEM((PARTS, depth, 2 * SUBS, bins // 2 // PARTS), jnp.bfloat16),
            dma((4,)),
            dma((PIECES,)),
            dma((2 * PLANE,)),
            dma((PLANE + 1,)),
            dma((PLANE - 1,)),
            dma((PLANE - 1,)),
            dma((PARTS, depth)),
            dma((PARTS, depth)),
        ],
        compiler_params=pltpu.CompilerParams(collective_id=0, has_side_effects=True),
    )(jitter.reshape(1, ang_dev), shift, sinogram, slab, base)


def solution(mesh):
    in_specs = (P("blk", "slab", None), P("blk"), P())
    out_specs = P("blk", "slab", None)
    return jax.shard_map(body, mesh=mesh, in_specs=in_specs, out_specs=out_specs, check_vma=False)
```

```python
import functools
import math

import jax
import jax.numpy as jnp
import numpy as np
from jax import lax
from jax.experimental import pallas as pl
from jax.experimental.pallas import tpu as pltpu
from jax.sharding import PartitionSpec as P

LANES = 128
SUBS = 8
BLOCK = 256
PLANE = 4
STEP = 64
JITTER = 0.29882812
SHIFT = 8
PIECES = 1
PARTS = 1
SENDS = (1, 2, 3)
MESH = pl.DeviceIdType.MESH


def ramp_slab(bins):
    span = bins // 2
    offset = np.arange(-span, span, dtype=np.int32)[None, :] - np.arange(LANES, dtype=np.int32)[:, None]
    safe = (2 * offset + 1).astype(np.float32)
    slab = (np.float32(-1.0) / (np.float32(math.pi**2) * safe * safe)).astype(jnp.bfloat16)
    return np.ascontiguousarray(slab.reshape(LANES, -1, LANES).transpose(1, 0, 2))


def window_base(width, ang_dev, rows_dev, bins):
    depth = width // PLANE
    angles, nrows = width * ang_dev, width * rows_dev
    nblocks, per = bins // LANES, PLANE * ang_dev
    groups = depth * rows_dev // SUBS
    half = (bins - 1) / 2
    me = np.arange(width)
    z, q = me // PLANE, me % PLANE
    a = z[:, None] * per + np.arange(per)[None, :]
    theta = (a[..., None] + np.linspace(-JITTER, JITTER, 9)) * math.pi / angles
    zs = np.arange(groups)[:, None] * (SUBS // rows_dev) + np.array([0, SUBS // rows_dev - 1])
    rows = (zs[None] * PLANE + q[:, None, None]) * rows_dev + np.array([0, rows_dev - 1])
    y = rows - (nrows - 1) / 2
    x = np.arange(nblocks)[:, None] * LANES + np.array([0, LANES - 1]) - half
    u = (
        x[None, None, :, None, :, None, None] * np.cos(theta)[:, :, None, None, None, None, :]
        + y[:, None, None, :, None, :, None] * np.sin(theta)[:, :, None, None, None, None, :]
        + half
    )
    low = np.floor(u.min(axis=(4, 5, 6)) - 0.25).astype(np.int32)
    high = u.max(axis=(4, 5, 6)) + 0.25
    assert (high - low).max() + STEP < 2 * LANES
    assert low.min() - SHIFT >= -STEP and low.max() + SHIFT < bins + STEP
    return (low + STEP).reshape(width, 1, per * nblocks * groups)


def lane_gather(x, index):
    dims = lax.GatherDimensionNumbers(
        offset_dims=(),
        collapsed_slice_dims=(1,),
        start_index_map=(1,),
        operand_batching_dims=(0,),
        start_indices_batching_dims=(0,),
    )
    return lax.gather(
        x, index[..., None], dims, (1, 1), mode=lax.GatherScatterMode.PROMISE_IN_BOUNDS
    )


def kernel(
    width,
    jit_hbm,
    shift_hbm,
    sino_hbm,
    slab_hbm,
    base_hbm,
    out_ref,
    jit_ref,
    shift_ref,
    sino_ref,
    slab,
    base,
    chunks,
    msgs,
    tab,
    held,
    fin,
    snd,
    rcv,
    lsem,
    wsem,
    sj,
    rj,
    s1,
    r1,
    s2,
    r2,
):
    me = lax.axis_index("blk")
    ang_dev, slices, bins = sino_ref.shape
    rows_dev = out_ref.shape[0]
    angles = width * ang_dev
    nrows = width * rows_dev
    nblocks = bins // LANES
    nspans = bins // BLOCK
    depth = width // PLANE
    groups = held.shape[2]
    zper = SUBS // rows_dev
    z, q = me // PLANE, me % PLANE
    half = (bins - 1) / 2

    def remote(src, dst, send, recv, dev):
        return pltpu.make_async_remote_copy(
            src_ref=src,
            dst_ref=dst,
            send_sem=send,
            recv_sem=recv,
            device_id={"blk": dev},
            device_id_type=MESH,
        )

    loads = [
        pltpu.make_async_copy(src, dst, lsem.at[i])
        for i, (src, dst) in enumerate(
            [
                (jit_hbm, jit_ref),
                (sino_hbm, sino_ref),
                (shift_hbm, shift_ref),
                (base_hbm.at[me], base),
            ]
        )
    ]
    kblocks = bins // 2 // BLOCK
    ntiles = slab.shape[0]
    cuts = [0]
    for piece in range(PIECES):
        cuts.append(2 + 2 * -(-(2 * kblocks - 1) * (piece + 1) // PIECES))
    weights = [
        pltpu.make_async_copy(
            slab_hbm.at[cuts[n] : cuts[n + 1]], slab.at[cuts[n] : cuts[n + 1]], wsem.at[n]
        )
        for n in range(PIECES)
    ]
    for load in loads[:2] + weights + loads[2:]:
        load.start()

    barrier = pltpu.get_barrier_semaphore()

    qx, qy = q % 2, q // 2
    ends = PLANE - 1

    def peer(d):
        return z * PLANE + (qx + d % 2) % 2 + 2 * ((qy + d // 2) % 2)

    def hello(dev):
        pl.semaphore_signal(barrier, inc=1, device_id={"blk": dev}, device_id_type=MESH)

    for d in (3, 1, 2):
        hello(peer(d))

    @pl.loop(1, depth)
    def _(k):
        hello((z + k) % depth * PLANE + q)

    @pl.when(q != ends)
    def _():
        hello((z + depth - 1) % depth * PLANE + ends)

    @pl.when((q != 0) & (z < depth - 1))
    def _():
        hello((z + 1) * PLANE)

    greeted = (
        ends + depth - 1
        + ends * (q // ends)
        + ends * ((PLANE - 1 - q) // ends) * ((z + depth - 1) // depth)
    )

    jrow = msgs.at[0, SUBS : 2 * SUBS]

    def jplane(d):
        return remote(msgs.at[0], msgs.at[d], sj.at[d - 1], rj.at[d - 1], peer(d))

    def jnext(p):
        return remote(
            jrow, msgs.at[PLANE, SUBS : 2 * SUBS], sj.at[PLANE - 1 + p], rj.at[PLANE - 1],
            (z + 1) % depth * PLANE + p,
        )

    def jprev(p):
        return remote(
            jrow, msgs.at[PLANE + 1, SUBS : 2 * SUBS], sj.at[PLANE - 1 + p], rj.at[PLANE],
            (z - 1) * PLANE + p,
        )

    def jwrap():
        return remote(
            msgs.at[q, SUBS : 2 * SUBS], msgs.at[PLANE + 1, SUBS : 2 * SUBS],
            sj.at[2 * PLANE - 1], rj.at[PLANE], (depth - 1) * PLANE + q,
        )

    def share(d):
        return remote(chunks.at[0], chunks.at[d], s1.at[d - 1], r1.at[d - 1], peer(d))

    def give(zt, part):
        return remote(
            snd.at[part, zt], rcv.at[part, z], s2.at[part, zt], r2.at[part, z], zt * PLANE + q
        )

    def take(zs, part):
        return remote(
            snd.at[part, zs], rcv.at[part, zs], s2.at[part, zs], r2.at[part, zs], zs * PLANE + q
        )

    lane = lax.broadcasted_iota(jnp.int32, (SUBS, LANES), 1)
    sub = lax.broadcasted_iota(jnp.int32, (SUBS, LANES), 0)
    lanef = lane.astype(jnp.float32)
    tab[tab.shape[0] - 1] = jnp.zeros((SUBS, LANES), jnp.int32)

    loads[0].wait()
    loads[1].wait()
    flat = jnp.concatenate(
        [sino_ref[i].astype(jnp.float32) for i in range(ang_dev)], axis=0
    )
    tiles = [flat[:, b * LANES : (b + 1) * LANES] for b in range(nblocks)]
    mine = (lane % angles) - me * ang_dev
    msg = jnp.zeros((SUBS, LANES), jnp.float32)
    for i in range(ang_dev):
        msg = jnp.where(mine == i, jit_ref[0:1, i : i + 1].astype(jnp.float32), msg)
    theta = ((lane % angles).astype(jnp.float32) + msg) * math.pi / angles
    waves = [jnp.cos(theta) * 0.5, jnp.sin(theta) * 0.5]
    rows = msg
    for i in range(ang_dev):
        pick = jnp.full((SUBS, LANES), me * ang_dev + i, jnp.int32)
        for n in range(2):
            rows = jnp.where(sub == 1 + 2 * i + n, lane_gather(waves[n], pick), rows)
    msgs[0, SUBS : 2 * SUBS] = rows

    top = jnp.abs(tiles[0])
    for tile in tiles[1:]:
        top = jnp.maximum(top, jnp.abs(tile))
    top = jnp.broadcast_to(jnp.max(top, axis=1, keepdims=True), (SUBS, LANES))
    msgs[0, :SUBS] = jnp.maximum(top, 1e-30) * (0.51 / 32700)

    def unzip(start):
        picked = [lane_gather(tile, (2 * lane + start) % LANES) for tile in tiles]
        at = 2 * lane + start
        outs = []
        for t in range(nspans):
            out = jnp.where(at < LANES, picked[2 * t], picked[2 * t + 1])
            if start < 0:
                out = jnp.where(at < 0, picked[2 * t - 1] if t else 0.0, out)
            outs.append(out)
        return outs

    evens, odds, late = unzip(0), unzip(1), unzip(-1)
    lhs = jnp.concatenate(
        [
            jnp.concatenate([part[2 * k], part[2 * k + 1]], axis=1)
            for part in (evens, late)
            for k in range(kblocks)
        ],
        axis=0,
    ).astype(jnp.bfloat16)
    rest = jnp.broadcast_to(odds[-1][:, LANES - 1 :], (SUBS, LANES))
    total = [[odds[t] * 0.25 for t in range(nspans)], [evens[t] * 0.25 for t in range(nspans)]]
    ready = 0
    for d in range(2 * kblocks - 1):
        while cuts[ready] < 2 * d + 4:
            weights[ready].wait()
            ready += 1
        up = jnp.concatenate([slab[2 * d + 2], slab[2 * d + 3]], axis=1)
        down = jnp.concatenate([slab[2 * d + 1], slab[2 * d + 2]], axis=1)
        prod = jnp.dot(
            lhs, jnp.concatenate([up, down], axis=0), preferred_element_type=jnp.float32
        )
        for p in range(2):
            for i in range(kblocks):
                j = d - (kblocks - 1) + i
                if 0 <= j < kblocks:
                    row = (p * kblocks + i) * SUBS
                    for n in range(2):
                        total[p][2 * j + n] = (
                            total[p][2 * j + n]
                            + prod[row : row + SUBS, n * LANES : (n + 1) * LANES]
                        )
    for t in range(nspans):
        ends_at = jnp.broadcast_to(slab[t, 0:1].astype(jnp.float32), (SUBS, LANES))
        total[1][t] = total[1][t] + rest * ends_at
    for t in range(nspans):
        chunks[0, :, t * LANES : (t + 1) * LANES] = jnp.concatenate(
            [total[1][t], total[0][t]], axis=0
        ).astype(jnp.bfloat16)

    pl.semaphore_wait(barrier, greeted)

    for d in SENDS:
        jplane(d).start()

    @pl.when(q == PLANE - 1)
    def _():
        for p in range(PLANE):
            jnext(p).start()

    @pl.when((q == 0) & (z > 0))
    def _():
        for p in range(PLANE):
            jprev(p).start()

    @pl.when((q == 0) & (z == 0))
    def _():
        jwrap().start()

    for d in SENDS:
        share(d).start()

    loads[2].wait()
    loads[3].wait()

    lead = sub % slices < slices // 2
    ypos = []
    for g in range(groups):
        row = ((sub % zper + g * zper) * PLANE + q) * rows_dev + sub // zper
        ypos.append(row.astype(jnp.float32) - (nrows - 1) / 2)

    def spread(d):
        inverse = 1.0 / msgs[d, :SUBS]
        words = []
        for t in range(nspans):
            both = chunks[d, :, t * LANES : (t + 1) * LANES].astype(jnp.float32)
            even = jnp.round(both[:SUBS] * inverse).astype(jnp.int32)
            odd = jnp.round(both[SUBS:] * inverse).astype(jnp.int32)
            high = jnp.where(lead, even, pltpu.roll(odd, 2, 0))
            low = jnp.where(lead, pltpu.roll(even, SUBS - 2, 0), odd)
            words.append(lax.shift_left(high, 16) + low)
            tab[4 * t + 1] = words[-1]
        for j in range(1, 4):
            cut = LANES - 32 * j
            turned = [pltpu.roll(word, cut, 1) for word in words]
            for t in range(nspans):
                after = turned[t + 1] if t + 1 < nspans else 0
                tab[4 * t + j + 1] = jnp.where(lane < cut, turned[t], after)
            if j == 3:
                tab[0] = jnp.where(lane < cut, 0, turned[0])

    def spoken(d, row):
        return jnp.broadcast_to(msgs[d, row : row + 1], (SUBS, LANES))

    def angle(d, i):
        cosb, sinb = (spoken(d, SUBS + 1 + 2 * i + n) for n in range(2))
        parts = [lanef * cosb + ypos[g] * sinb for g in range(groups)]
        scales = [spoken(d, i * slices + s) * (1.0 / 65536) for s in range(slices)]
        return cosb, parts, scales

    def line(slot, row):
        return jnp.broadcast_to(tab[slot, row : row + 1], (SUBS, LANES))

    def project(d, known, g, b):
        pc = peer(d)
        qc = pc - z * PLANE
        sums = []
        for i in range(ang_dev):
            cosb, parts, scales = known[i]
            moved = shift_ref[pc * ang_dev + i]
            slot = base[0, ((qc * ang_dev + i) * nblocks + b) * groups + g]
            slot = lax.shift_right_arithmetic(slot + moved, 6)
            offset = (moved - slot * STEP).astype(jnp.float32) * 0.5 + (half + STEP) * 0.5
            h = cosb * (b * LANES - half) + parts[g] + offset
            odd = h.astype(jnp.int32)
            even = (h + 0.5).astype(jnp.int32)
            frac = jnp.abs(h - even.astype(jnp.float32)) * 2.0
            pairs = slices // 2
            evens = [lane_gather(line(slot, i * slices + s), even) for s in range(pairs)]
            odds = [lane_gather(line(slot, i * slices + pairs + s), odd) for s in range(pairs)]
            got = []
            for s in range(slices):
                e, o = evens[s % pairs], odds[s % pairs]
                if s >= pairs:
                    e, o = lax.shift_left(e, 16), lax.shift_left(o, 16)
                e, o = e.astype(jnp.float32), o.astype(jnp.float32)
                got.append((e + frac * (o - e)) * scales[s])
            sums.append(got)
        return sums

    def keep(d):
        spread(d)
        known = [angle(d, i) for i in range(ang_dev)]
        for b in range(nblocks):
            for g in range(groups):
                for i, got in enumerate(project(d, known, g, b)):
                    for s in range(slices):
                        held[d, i, g, s, b] = got[s]

    keep(0)

    @pl.when((q > 0) & (z == 0))
    def _():
        jplane(q).wait_recv()
        jwrap().start()

    @pl.loop(1, PLANE - 1)
    def _(d):
        @pl.when((z > 0) | (q != d))
        def _():
            jplane(d).wait_recv()

        share(d).wait_recv()
        keep(d)

    d = PLANE - 1

    @pl.when((z > 0) | (q != d))
    def _():
        jplane(d).wait_recv()

    jnext(0).wait_recv()
    jprev(0).wait_recv()
    share(d).wait_recv()
    jit = sum(spoken(i, SUBS) for i in range(PLANE + 2))
    ahead = pltpu.roll(jit, LANES - 1, 1)
    behind = pltpu.roll(jit, 1, 1)
    weight = (1.0 + (ahead - behind) * 1.5) * (4.0 / math.sqrt(angles))
    weight = [
        [
            lane_gather(weight, jnp.full((SUBS, LANES), peer(n) * ang_dev + i, jnp.int32))
            for i in range(ang_dev)
        ]
        for n in range(PLANE)
    ]
    spread(d)
    known = [angle(d, i) for i in range(ang_dev)]
    pos = sub % zper
    ntile = nblocks // 2 // PARTS
    for part in range(PARTS):
        for t in range(ntile):
            for g in range(groups):
                out = [[], [], [], []]
                for b in (2 * (part * ntile + t), 2 * (part * ntile + t) + 1):
                    got = project(d, known, g, b)
                    v = []
                    for s in range(slices):
                        terms = [weight[d][i] * got[i][s] for i in range(ang_dev)]
                        for n in range(PLANE - 1):
                            terms += [weight[n][i] * held[n, i, g, s, b] for i in range(ang_dev)]
                        while len(terms) > 1:
                            terms = [x + y for x, y in zip(terms[::2], terms[1::2])]
                        v += terms
                    w = [None] * 4
                    for s in range(2):
                        w[s] = jnp.where(pos < 2, v[s], pltpu.roll(v[s + 2], 2, 0))
                        w[s + 2] = jnp.where(pos < 2, pltpu.roll(v[s], SUBS - 2, 0), v[s + 2])
                    for s in (0, 2):
                        lo = jnp.where(pos % 2 < 1, w[s], pltpu.roll(w[s + 1], 1, 0))
                        hi = jnp.where(pos % 2 < 1, pltpu.roll(w[s], SUBS - 1, 0), w[s + 1])
                        for n, val in ((s, lo), (s + 1, hi)):
                            fin[g * zper + n, b] = val
                            out[n].append(val)
                for n in range(4):
                    snd[part, g * zper + n, :, t * LANES : (t + 1) * LANES] = jnp.concatenate(
                        out[n], axis=0
                    ).astype(jnp.bfloat16)

        @pl.loop(0, depth)
        def _(zt):
            @pl.when(zt != z)
            def _():
                give(zt, part).start()

    for part in range(PARTS):
        @pl.loop(1, depth)
        def _(k):
            take((z + k) % depth, part).wait_recv()

        for t in range(ntile):
            b = 2 * (part * ntile + t)
            sums = [fin[z, b], fin[z, b + 1]]
            for k in range(1, depth):
                both = rcv[part, (z + k) % depth, :, t * LANES : (t + 1) * LANES]
                both = both.astype(jnp.float32)
                sums = [sums[0] + both[:SUBS], sums[1] + both[SUBS:]]
            for j in range(2):
                cols = slice((b + j) * LANES, (b + j + 1) * LANES)
                for r in range(rows_dev):
                    out_ref[r, :, cols] = sums[j][r * slices : (r + 1) * slices]

    for d in range(1, PLANE):
        jplane(d).wait_send()
        share(d).wait_send()

    @pl.when(q == PLANE - 1)
    def _():
        for p in range(PLANE):
            jnext(p).wait_send()

    @pl.when((q == 0) & (z > 0))
    def _():
        for p in range(PLANE):
            jprev(p).wait_send()

    @pl.when(z == 0)
    def _():
        jwrap().wait_send()

    for part in range(PARTS):
        @pl.loop(1, depth)
        def _(k):
            give((z + k) % depth, part).wait_send()


def body(sinogram, jitter, shift):
    width = lax.axis_size("blk")
    ang_dev, slices, bins = sinogram.shape
    angles = shift.shape[0]
    rows_dev = SUBS // slices
    depth = width // PLANE
    assert ang_dev == 2 and rows_dev == 2 and slices == 4 and LANES % angles == 0
    assert width % (PLANE * 4) == 0 and bins % (2 * BLOCK) == 0
    groups = depth * rows_dev // SUBS
    nblocks = bins // LANES
    anywhere = pl.BlockSpec(memory_space=pl.ANY)
    dma = pltpu.SemaphoreType.DMA
    slab = jnp.asarray(ramp_slab(bins))
    base = jnp.asarray(window_base(width, ang_dev, rows_dev, bins))
    return pl.pallas_call(
        functools.partial(kernel, width),
        out_shape=pltpu.VMEM((rows_dev, slices, bins), jnp.float32),
        in_specs=[anywhere] * 5,
        out_specs=pl.BlockSpec(memory_space=pltpu.VMEM),
        scratch_shapes=[
            pltpu.VMEM((1, ang_dev), jnp.bfloat16),
            pltpu.SMEM((angles,), jnp.int32),
            pltpu.VMEM((ang_dev, slices, bins), jnp.bfloat16),
            pltpu.VMEM(slab.shape, jnp.bfloat16),
            pltpu.SMEM(base.shape[1:], jnp.int32),
            pltpu.VMEM((PLANE, 2 * SUBS, bins // 2), jnp.bfloat16),
            pltpu.VMEM((PLANE + 2, 2 * SUBS, LANES), jnp.float32),
            pltpu.VMEM((bins // STEP + 2, SUBS, LANES), jnp.int32),
            pltpu.VMEM((PLANE - 1, ang_dev, groups, slices, nblocks, SUBS, LANES), jnp.float32),
            pltpu.VMEM((depth, nblocks, SUBS, LANES), jnp.float32),
            pltpu.VMEM((PARTS, depth, 2 * SUBS, bins // 2 // PARTS), jnp.bfloat16),
            pltpu.VMEM((PARTS, depth, 2 * SUBS, bins // 2 // PARTS), jnp.bfloat16),
            dma((4,)),
            dma((PIECES,)),
            dma((2 * PLANE,)),
            dma((PLANE + 1,)),
            dma((PLANE - 1,)),
            dma((PLANE - 1,)),
            dma((PARTS, depth)),
            dma((PARTS, depth)),
        ],
        compiler_params=pltpu.CompilerParams(collective_id=0, has_side_effects=True),
    )(jitter.reshape(1, ang_dev), shift, sinogram, slab, base)


def solution(mesh):
    in_specs = (P("blk", "slab", None), P("blk"), P())
    out_specs = P("blk", "slab", None)
    return jax.shard_map(body, mesh=mesh, in_specs=in_specs, out_specs=out_specs, check_vma=False)
```

```python
import functools
import math

import jax
import jax.numpy as jnp
import numpy as np
from jax import lax
from jax.experimental import pallas as pl
from jax.experimental.pallas import tpu as pltpu
from jax.sharding import PartitionSpec as P

LANES = 128
SUBS = 8
BLOCK = 256
PLANE = 4
STEP = 64
JITTER = 0.29882812
SHIFT = 8
SENDS = (1, 2, 3)
GATHERS = [(i, p, s) for i in (0, 1) for p, s in ((0, 0), (1, 0), (1, 1), (0, 1))]
MESH = pl.DeviceIdType.MESH


def ramp_slab(bins):
    span = bins // 2
    offset = np.arange(-span, span, dtype=np.int32)[None, :] - np.arange(LANES, dtype=np.int32)[:, None]
    safe = (2 * offset + 1).astype(np.float32)
    slab = (np.float32(-1.0) / (np.float32(math.pi**2) * safe * safe)).astype(jnp.bfloat16)
    return np.ascontiguousarray(slab.reshape(LANES, -1, LANES).transpose(1, 0, 2))


def window_base(width, ang_dev, rows_dev, bins):
    depth = width // PLANE
    angles, nrows = width * ang_dev, width * rows_dev
    nblocks, per = bins // LANES, PLANE * ang_dev
    groups = depth * rows_dev // SUBS
    half = (bins - 1) / 2
    me = np.arange(width)
    z, q = me // PLANE, me % PLANE
    a = z[:, None] * per + np.arange(per)[None, :]
    theta = (a[..., None] + np.linspace(-JITTER, JITTER, 9)) * math.pi / angles
    zs = np.arange(groups)[:, None] * (SUBS // rows_dev) + np.array([0, SUBS // rows_dev - 1])
    rows = (zs[None] * PLANE + q[:, None, None]) * rows_dev + np.array([0, rows_dev - 1])
    y = rows - (nrows - 1) / 2
    x = np.arange(nblocks)[:, None] * LANES + np.array([0, LANES - 1]) - half
    u = (
        x[None, None, :, None, :, None, None] * np.cos(theta)[:, :, None, None, None, None, :]
        + y[:, None, None, :, None, :, None] * np.sin(theta)[:, :, None, None, None, None, :]
        + half
    )
    low = np.floor(u.min(axis=(4, 5, 6)) - 0.25).astype(np.int32)
    high = u.max(axis=(4, 5, 6)) + 0.25
    assert (high - low).max() + STEP < 2 * LANES
    assert low.min() - SHIFT >= -STEP and low.max() + SHIFT < bins + STEP
    return (low + STEP).reshape(width, 1, per * nblocks * groups)


def lane_gather(x, index):
    dims = lax.GatherDimensionNumbers(
        offset_dims=(),
        collapsed_slice_dims=(1,),
        start_index_map=(1,),
        operand_batching_dims=(0,),
        start_indices_batching_dims=(0,),
    )
    return lax.gather(
        x, index[..., None], dims, (1, 1), mode=lax.GatherScatterMode.PROMISE_IN_BOUNDS
    )


def kernel(
    width,
    jit_hbm,
    shift_hbm,
    sino_hbm,
    slab_hbm,
    base_hbm,
    out_ref,
    jit_ref,
    shift_ref,
    sino_ref,
    slab,
    base,
    chunks,
    msgs,
    tab,
    held,
    fin,
    snd,
    rcv,
    lsem,
    wsem,
    sj,
    rj,
    s1,
    r1,
    s2,
    r2,
):
    me = lax.axis_index("blk")
    ang_dev, slices, bins = sino_ref.shape
    rows_dev = out_ref.shape[0]
    angles = width * ang_dev
    nrows = width * rows_dev
    nblocks = bins // LANES
    nspans = bins // BLOCK
    depth = width // PLANE
    groups = held.shape[2]
    zper = SUBS // rows_dev
    z, q = me // PLANE, me % PLANE
    half = (bins - 1) / 2

    def remote(src, dst, send, recv, dev):
        return pltpu.make_async_remote_copy(
            src_ref=src,
            dst_ref=dst,
            send_sem=send,
            recv_sem=recv,
            device_id={"blk": dev},
            device_id_type=MESH,
        )

    loads = [
        pltpu.make_async_copy(src, dst, lsem.at[i])
        for i, (src, dst) in enumerate(
            [
                (jit_hbm, jit_ref),
                (sino_hbm, sino_ref),
                (shift_hbm, shift_ref),
                (base_hbm.at[me], base),
            ]
        )
    ]
    kblocks = bins // 2 // BLOCK
    weights = [pltpu.make_async_copy(slab_hbm, slab, wsem.at[0])]
    for load in [loads[1], loads[0]] + weights + loads[2:]:
        load.start()

    barrier = pltpu.get_barrier_semaphore()

    qx, qy = q % 2, q // 2
    ends = PLANE - 1

    def peer(d):
        return z * PLANE + (qx + d % 2) % 2 + 2 * ((qy + d // 2) % 2)

    def hello(dev):
        pl.semaphore_signal(barrier, inc=1, device_id={"blk": dev}, device_id_type=MESH)

    for d in (3, 1, 2):
        hello(peer(d))

    @pl.loop(1, depth)
    def _(k):
        hello((z + k) % depth * PLANE + q)

    @pl.when(q != ends)
    def _():
        hello((z + depth - 1) % depth * PLANE + ends)

    @pl.when((q != 0) & (z < depth - 1))
    def _():
        hello((z + 1) * PLANE)

    greeted = (
        ends + depth - 1
        + ends * (q // ends)
        + ends * ((PLANE - 1 - q) // ends) * ((z + depth - 1) // depth)
    )

    jrow = msgs.at[0, SUBS : 2 * SUBS]

    def jplane(d):
        return remote(msgs.at[0], msgs.at[d], sj.at[d - 1], rj.at[d - 1], peer(d))

    def jnext(p):
        return remote(
            jrow, msgs.at[PLANE, SUBS : 2 * SUBS], lsem.at[p], rj.at[PLANE - 1],
            (z + 1) % depth * PLANE + p,
        )

    def jprev(p):
        return remote(
            jrow, msgs.at[PLANE + 1, SUBS : 2 * SUBS], lsem.at[p], rj.at[PLANE],
            (z - 1) * PLANE + p,
        )

    def jwrap():
        return remote(
            msgs.at[q, SUBS : 2 * SUBS], msgs.at[PLANE + 1, SUBS : 2 * SUBS],
            wsem.at[0], rj.at[PLANE], (depth - 1) * PLANE + q,
        )

    def share(d):
        return remote(chunks.at[0], chunks.at[d], s1.at[d - 1], r1.at[d - 1], peer(d))

    def give(zt):
        k = (zt - z + depth) % depth
        return remote(snd.at[zt], rcv.at[k - 1], s2.at[k - 1], r2.at[k - 1], zt * PLANE + q)

    def take(k):
        return remote(
            snd.at[0], rcv.at[k - 1], s2.at[k - 1], r2.at[k - 1],
            (z + depth - k) % depth * PLANE + q,
        )

    lane = lax.broadcasted_iota(jnp.int32, (SUBS, LANES), 1)
    sub = lax.broadcasted_iota(jnp.int32, (SUBS, LANES), 0)
    lanef = lane.astype(jnp.float32)
    tab[tab.shape[0] - 1] = jnp.zeros((SUBS, LANES), jnp.int32)

    loads[0].wait()
    loads[1].wait()
    flat = jnp.concatenate(
        [sino_ref[i].astype(jnp.float32) for i in range(ang_dev)], axis=0
    )
    tiles = [flat[:, b * LANES : (b + 1) * LANES] for b in range(nblocks)]
    def unzip(start):
        picked = [lane_gather(tile, (2 * lane + start) % LANES) for tile in tiles]
        at = 2 * lane + start
        outs = []
        for t in range(nspans):
            out = jnp.where(at < LANES, picked[2 * t], picked[2 * t + 1])
            if start < 0:
                out = jnp.where(at < 0, picked[2 * t - 1] if t else 0.0, out)
            outs.append(out)
        return outs

    evens, odds, late = unzip(0), unzip(1), unzip(-1)
    lhs = jnp.concatenate(
        [
            jnp.concatenate([part[2 * k], part[2 * k + 1]], axis=1)
            for part in (evens, late)
            for k in range(kblocks)
        ],
        axis=0,
    ).astype(jnp.bfloat16)
    weights[0].wait()
    mine = (lane % angles) - me * ang_dev
    msg = jnp.zeros((SUBS, LANES), jnp.float32)
    for i in range(ang_dev):
        msg = jnp.where(mine == i, jit_ref[0:1, i : i + 1].astype(jnp.float32), msg)
    theta = ((lane % angles).astype(jnp.float32) + msg) * math.pi / angles
    waves = [jnp.cos(theta) * 0.5, jnp.sin(theta) * 0.5]
    rows = msg
    for i in range(ang_dev):
        pick = jnp.full((SUBS, LANES), me * ang_dev + i, jnp.int32)
        for n in range(2):
            rows = jnp.where(sub == 1 + 2 * i + n, lane_gather(waves[n], pick), rows)
    msgs[0, SUBS : 2 * SUBS] = rows

    top = jnp.abs(tiles[0])
    for tile in tiles[1:]:
        top = jnp.maximum(top, jnp.abs(tile))
    top = jnp.broadcast_to(jnp.max(top, axis=1, keepdims=True), (SUBS, LANES))
    msgs[0, :SUBS] = jnp.maximum(top, 1e-30) * (0.51 / 32700)

    rest = jnp.broadcast_to(odds[-1][:, LANES - 1 :], (SUBS, LANES))
    total = [[odds[t] * 0.25 for t in range(nspans)], [evens[t] * 0.25 for t in range(nspans)]]
    for d in range(2 * kblocks - 1):
        up = jnp.concatenate([slab[2 * d + 2], slab[2 * d + 3]], axis=1)
        down = jnp.concatenate([slab[2 * d + 1], slab[2 * d + 2]], axis=1)
        prod = jnp.dot(
            lhs, jnp.concatenate([up, down], axis=0), preferred_element_type=jnp.float32
        )
        for p in range(2):
            for i in range(kblocks):
                j = d - (kblocks - 1) + i
                if 0 <= j < kblocks:
                    row = (p * kblocks + i) * SUBS
                    for n in range(2):
                        total[p][2 * j + n] = (
                            total[p][2 * j + n]
                            + prod[row : row + SUBS, n * LANES : (n + 1) * LANES]
                        )
    for t in range(nspans):
        ends_at = jnp.broadcast_to(slab[t, 0:1].astype(jnp.float32), (SUBS, LANES))
        total[1][t] = total[1][t] + rest * ends_at
    for t in range(nspans):
        chunks[0, :, t * LANES : (t + 1) * LANES] = jnp.concatenate(
            [total[1][t], total[0][t]], axis=0
        ).astype(jnp.bfloat16)

    loads[2].wait()
    loads[3].wait()
    pl.semaphore_wait(barrier, greeted)

    for d in SENDS:
        jplane(d).start()

    @pl.when((q == 0) & (z == 0))
    def _():
        jwrap().start()

    for d in SENDS:
        share(d).start()


    @pl.when(q == PLANE - 1)
    def _():
        for p in range(PLANE):
            jnext(p).start()

    @pl.when((q == 0) & (z > 0))
    def _():
        for p in range(PLANE):
            jprev(p).start()


    lead = sub % slices < slices // 2
    ypos = []
    for g in range(groups):
        row = ((sub % zper + g * zper) * PLANE + q) * rows_dev + sub // zper
        ypos.append(row.astype(jnp.float32) - (nrows - 1) / 2)

    def spread(d):
        inverse = 1.0 / msgs[d, :SUBS]
        words = []
        for t in range(nspans):
            both = chunks[d, :, t * LANES : (t + 1) * LANES].astype(jnp.float32)
            even = jnp.round(both[:SUBS] * inverse).astype(jnp.int32)
            odd = jnp.round(both[SUBS:] * inverse).astype(jnp.int32)
            high = jnp.where(lead, even, pltpu.roll(odd, 2, 0))
            low = jnp.where(lead, pltpu.roll(even, SUBS - 2, 0), odd)
            words.append(lax.shift_left(high, 16) + low)
            tab[4 * t + 1] = words[-1]
        for j in range(1, 4):
            cut = LANES - 32 * j
            turned = [pltpu.roll(word, cut, 1) for word in words]
            for t in range(nspans):
                after = turned[t + 1] if t + 1 < nspans else 0
                tab[4 * t + j + 1] = jnp.where(lane < cut, turned[t], after)
            if j == 3:
                tab[0] = jnp.where(lane < cut, 0, turned[0])

    def spoken(d, row):
        return jnp.broadcast_to(msgs[d, row : row + 1], (SUBS, LANES))

    def angle(d, i):
        cosb, sinb = (spoken(d, SUBS + 1 + 2 * i + n) for n in range(2))
        parts = [lanef * cosb + ypos[g] * sinb for g in range(groups)]
        scales = [spoken(d, i * slices + s) * (1.0 / 65536) for s in range(slices)]
        return cosb, parts, scales

    def line(slot, row):
        return jnp.broadcast_to(tab[slot, row : row + 1], (SUBS, LANES))

    def project(d, known, g, b):
        pc = peer(d)
        qc = pc - z * PLANE
        pairs = slices // 2
        index, fracs, slots = [], [], []
        for i in range(ang_dev):
            cosb, parts, scales = known[i]
            moved = shift_ref[pc * ang_dev + i]
            slot = base[0, ((qc * ang_dev + i) * nblocks + b) * groups + g]
            slot = lax.shift_right_arithmetic(slot + moved, 6)
            offset = (moved - slot * STEP).astype(jnp.float32) * 0.5 + (half + STEP) * 0.5
            h = cosb * (b * LANES - half) + parts[g] + offset
            odd = h.astype(jnp.int32)
            even = (h + 0.5).astype(jnp.int32)
            fracs.append(jnp.abs(h - even.astype(jnp.float32)) * 2.0)
            index.append((even, odd))
            slots.append(slot)
        words = {}
        for i, p, s in GATHERS:
            words[i, p, s] = lane_gather(line(slots[i], i * slices + p * pairs + s), index[i][p])
        sums = []
        for i in range(ang_dev):
            got = []
            for s in range(slices):
                e, o = words[i, 0, s % pairs], words[i, 1, s % pairs]
                if s >= pairs:
                    e, o = lax.shift_left(e, 16), lax.shift_left(o, 16)
                e, o = e.astype(jnp.float32), o.astype(jnp.float32)
                got.append((e + fracs[i] * (o - e)) * known[i][2][s])
            sums.append(got)
        return sums

    def keep(d):
        spread(d)
        known = [angle(d, i) for i in range(ang_dev)]
        for b in range(nblocks):
            for g in range(groups):
                for i, got in enumerate(project(d, known, g, b)):
                    for s in range(slices):
                        held[d, i, g, s, b] = got[s]

    keep(0)

    @pl.when((q > 0) & (z == 0))
    def _():
        jplane(q).wait_recv()
        jwrap().start()

    @pl.loop(1, PLANE - 1)
    def _(d):
        @pl.when((z > 0) | (q != d))
        def _():
            jplane(d).wait_recv()

        share(d).wait_recv()
        keep(d)

    d = PLANE - 1

    @pl.when((z > 0) | (q != d))
    def _():
        jplane(d).wait_recv()

    def weigh():
        jnext(0).wait_recv()
        jprev(0).wait_recv()
        jit = sum(spoken(i, SUBS) for i in range(PLANE + 2))
        ahead = pltpu.roll(jit, LANES - 1, 1)
        behind = pltpu.roll(jit, 1, 1)
        weight = (1.0 + (ahead - behind) * 1.5) * (4.0 / math.sqrt(angles))
        return [
            [
                lane_gather(weight, jnp.full((SUBS, LANES), peer(n) * ang_dev + i, jnp.int32))
                for i in range(ang_dev)
            ]
            for n in range(PLANE)
        ]

    def merge(weight, g, s, b, chunks_in):
        terms = [
            weight[n][i] * held[n, i, g, s, b] for n in chunks_in for i in range(ang_dev)
        ]
        while len(terms) > 1:
            terms = [x + y for x, y in zip(terms[::2], terms[1::2])] + terms[len(terms) // 2 * 2 :]
        return terms[0]

    pos = sub % zper

    def pack(rows_of):
        for t in range(nblocks // 2):
            for g in range(groups):
                out = [[], [], [], []]
                for b in (2 * t, 2 * t + 1):
                    v = rows_of(g, b)
                    w = [None] * 4
                    for s in range(2):
                        w[s] = jnp.where(pos < 2, v[s], pltpu.roll(v[s + 2], 2, 0))
                        w[s + 2] = jnp.where(pos < 2, pltpu.roll(v[s], SUBS - 2, 0), v[s + 2])
                    for s in (0, 2):
                        lo = jnp.where(pos % 2 < 1, w[s], pltpu.roll(w[s + 1], 1, 0))
                        hi = jnp.where(pos % 2 < 1, pltpu.roll(w[s], SUBS - 1, 0), w[s + 1])
                        for n, val in ((s, lo), (s + 1, hi)):
                            fin[g * zper + n, b] = val
                            out[n].append(val)
                for n in range(4):
                    snd[g * zper + n, :, t * LANES : (t + 1) * LANES] = jnp.concatenate(
                        out[n], axis=0
                    ).astype(jnp.bfloat16)

    waits_last = (z == depth - 1) & (q > 0)

    @pl.when(waits_last)
    def _():
        share(d).wait_recv()
        keep(d)
        weight = weigh()
        pack(lambda g, b: [merge(weight, g, s, b, range(PLANE)) for s in range(slices)])

    @pl.when(jnp.logical_not(waits_last))
    def _():
        weight = weigh()
        for b in range(nblocks):
            for g in range(groups):
                for s in range(slices):
                    held[0, 0, g, s, b] = merge(weight, g, s, b, range(PLANE - 1))
        share(d).wait_recv()
        spread(d)
        known = [angle(d, i) for i in range(ang_dev)]

        def rows_of(g, b):
            got = project(d, known, g, b)
            return [
                held[0, 0, g, s, b] + (weight[d][0] * got[0][s] + weight[d][1] * got[1][s])
                for s in range(slices)
            ]

        pack(rows_of)

    for n in range(1, PLANE):
        jplane(n).wait_send()
        share(n).wait_send()

    @pl.loop(0, depth)
    def _(zt):
        @pl.when(zt != z)
        def _():
            give(zt).start()

    @pl.when(q == ends)
    def _():
        for p in range(PLANE):
            jnext(p).wait_send()

    @pl.when((q == 0) & (z > 0))
    def _():
        for p in range(PLANE):
            jprev(p).wait_send()

    @pl.when(z == 0)
    def _():
        jwrap().wait_send()

    @pl.loop(1, depth)
    def _(k):
        take(k).wait_recv()

    for t in range(nblocks // 2):
        sums = [fin[z, 2 * t], fin[z, 2 * t + 1]]
        for k in range(1, depth):
            both = rcv[k - 1, :, t * LANES : (t + 1) * LANES].astype(jnp.float32)
            sums = [sums[0] + both[:SUBS], sums[1] + both[SUBS:]]
        for j in range(2):
            cols = slice((2 * t + j) * LANES, (2 * t + j + 1) * LANES)
            for r in range(rows_dev):
                out_ref[r, :, cols] = sums[j][r * slices : (r + 1) * slices]

    @pl.loop(1, depth)
    def _(k):
        give((z + k) % depth).wait_send()


def body(sinogram, jitter, shift):
    width = lax.axis_size("blk")
    ang_dev, slices, bins = sinogram.shape
    angles = shift.shape[0]
    rows_dev = SUBS // slices
    depth = width // PLANE
    assert ang_dev == 2 and rows_dev == 2 and slices == 4 and LANES % angles == 0
    assert width % (PLANE * 4) == 0 and bins % (2 * BLOCK) == 0
    groups = depth * rows_dev // SUBS
    nblocks = bins // LANES
    anywhere = pl.BlockSpec(memory_space=pl.ANY)
    dma = pltpu.SemaphoreType.DMA
    slab = jnp.asarray(ramp_slab(bins))
    base = jnp.asarray(window_base(width, ang_dev, rows_dev, bins))
    return pl.pallas_call(
        functools.partial(kernel, width),
        out_shape=pltpu.VMEM((rows_dev, slices, bins), jnp.float32),
        in_specs=[anywhere] * 5,
        out_specs=pl.BlockSpec(memory_space=pltpu.VMEM),
        scratch_shapes=[
            pltpu.VMEM((1, ang_dev), jnp.bfloat16),
            pltpu.SMEM((angles,), jnp.int32),
            pltpu.VMEM((ang_dev, slices, bins), jnp.bfloat16),
            pltpu.VMEM(slab.shape, jnp.bfloat16),
            pltpu.SMEM(base.shape[1:], jnp.int32),
            pltpu.VMEM((PLANE, 2 * SUBS, bins // 2), jnp.bfloat16),
            pltpu.VMEM((PLANE + 2, 2 * SUBS, LANES), jnp.float32),
            pltpu.VMEM((bins // STEP + 2, SUBS, LANES), jnp.int32),
            pltpu.VMEM((PLANE, ang_dev, groups, slices, nblocks, SUBS, LANES), jnp.float32),
            pltpu.VMEM((depth, nblocks, SUBS, LANES), jnp.float32),
            pltpu.VMEM((depth, 2 * SUBS, bins // 2), jnp.bfloat16),
            pltpu.VMEM((depth - 1, 2 * SUBS, bins // 2), jnp.bfloat16),
            dma((4,)),
            dma((1,)),
            dma((PLANE - 1,)),
            dma((PLANE + 1,)),
            dma((PLANE - 1,)),
            dma((PLANE - 1,)),
            dma((depth - 1,)),
            dma((depth - 1,)),
        ],
        compiler_params=pltpu.CompilerParams(collective_id=0, has_side_effects=True),
    )(jitter.reshape(1, ang_dev), shift, sinogram, slab, base)


def solution(mesh):
    in_specs = (P("blk", "slab", None), P("blk"), P())
    out_specs = P("blk", "slab", None)
    return jax.shard_map(body, mesh=mesh, in_specs=in_specs, out_specs=out_specs, check_vma=False)
```

```python
import functools
import math

import jax
import jax.numpy as jnp
import numpy as np
from jax import lax
from jax.experimental import pallas as pl
from jax.experimental.pallas import tpu as pltpu
from jax.sharding import PartitionSpec as P

LANES = 128
SUBS = 8
BLOCK = 256
PLANE = 4
STEP = 64
JITTER = 0.29882812
SHIFT = 8
SENDS = (1, 3, 2)
GATHERS = [(i, p, s) for i in (0, 1) for p, s in ((0, 0), (1, 0), (1, 1), (0, 1))]
MESH = pl.DeviceIdType.MESH


def ramp_slab(bins):
    span = bins // 2
    offset = np.arange(-span, span, dtype=np.int32)[None, :] - np.arange(LANES, dtype=np.int32)[:, None]
    safe = (2 * offset + 1).astype(np.float32)
    slab = (np.float32(-1.0) / (np.float32(math.pi**2) * safe * safe)).astype(jnp.bfloat16)
    return np.ascontiguousarray(slab.reshape(LANES, -1, LANES).transpose(1, 0, 2))


def window_base(width, ang_dev, rows_dev, bins):
    depth = width // PLANE
    angles, nrows = width * ang_dev, width * rows_dev
    nblocks, per = bins // LANES, PLANE * ang_dev
    groups = depth * rows_dev // SUBS
    half = (bins - 1) / 2
    me = np.arange(width)
    z, q = me // PLANE, me % PLANE
    a = z[:, None] * per + np.arange(per)[None, :]
    theta = (a[..., None] + np.linspace(-JITTER, JITTER, 9)) * math.pi / angles
    zs = np.arange(groups)[:, None] * (SUBS // rows_dev) + np.array([0, SUBS // rows_dev - 1])
    rows = (zs[None] * PLANE + q[:, None, None]) * rows_dev + np.array([0, rows_dev - 1])
    y = rows - (nrows - 1) / 2
    x = np.arange(nblocks)[:, None] * LANES + np.array([0, LANES - 1]) - half
    u = (
        x[None, None, :, None, :, None, None] * np.cos(theta)[:, :, None, None, None, None, :]
        + y[:, None, None, :, None, :, None] * np.sin(theta)[:, :, None, None, None, None, :]
        + half
    )
    low = np.floor(u.min(axis=(4, 5, 6)) - 0.25).astype(np.int32)
    high = u.max(axis=(4, 5, 6)) + 0.25
    assert (high - low).max() + STEP < 2 * LANES
    assert low.min() - SHIFT >= -STEP and low.max() + SHIFT < bins + STEP
    return (low + STEP).reshape(width, 1, per * nblocks * groups)


def lane_gather(x, index):
    dims = lax.GatherDimensionNumbers(
        offset_dims=(),
        collapsed_slice_dims=(1,),
        start_index_map=(1,),
        operand_batching_dims=(0,),
        start_indices_batching_dims=(0,),
    )
    return lax.gather(
        x, index[..., None], dims, (1, 1), mode=lax.GatherScatterMode.PROMISE_IN_BOUNDS
    )


def kernel(
    width,
    jit_hbm,
    shift_hbm,
    sino_hbm,
    slab_hbm,
    base_hbm,
    out_ref,
    jit_ref,
    shift_ref,
    sino_ref,
    slab,
    base,
    chunks,
    msgs,
    both_tabs,
    held,
    fin,
    snd,
    rcv,
    lsem,
    wsem,
    sj,
    rj,
    s1,
    r1,
    s2,
    r2,
):
    me = lax.axis_index("blk")
    ang_dev, slices, bins = sino_ref.shape
    rows_dev = out_ref.shape[0]
    angles = width * ang_dev
    nrows = width * rows_dev
    nblocks = bins // LANES
    nspans = bins // BLOCK
    depth = width // PLANE
    groups = held.shape[2]
    zper = SUBS // rows_dev
    z, q = me // PLANE, me % PLANE
    half = (bins - 1) / 2

    def remote(src, dst, send, recv, dev):
        return pltpu.make_async_remote_copy(
            src_ref=src,
            dst_ref=dst,
            send_sem=send,
            recv_sem=recv,
            device_id={"blk": dev},
            device_id_type=MESH,
        )

    loads = [
        pltpu.make_async_copy(src, dst, lsem.at[i])
        for i, (src, dst) in enumerate(
            [
                (jit_hbm, jit_ref),
                (sino_hbm, sino_ref),
                (shift_hbm, shift_ref),
                (base_hbm.at[me], base),
            ]
        )
    ]
    kblocks = bins // 2 // BLOCK
    weights = [pltpu.make_async_copy(slab_hbm, slab, wsem.at[0])]
    for load in [loads[1], loads[0]] + weights + loads[2:]:
        load.start()

    barrier = pltpu.get_barrier_semaphore()

    qx, qy = q % 2, q // 2
    ends = PLANE - 1

    def peer(d):
        return z * PLANE + (qx + d % 2) % 2 + 2 * ((qy + d // 2) % 2)

    def hello(dev):
        pl.semaphore_signal(barrier, inc=1, device_id={"blk": dev}, device_id_type=MESH)

    for d in (3, 1, 2):
        hello(peer(d))

    @pl.loop(1, depth)
    def _(k):
        hello((z + k) % depth * PLANE + q)

    @pl.when(q != ends)
    def _():
        hello((z + depth - 1) % depth * PLANE + ends)

    @pl.when((q != 0) & (z < depth - 1))
    def _():
        hello((z + 1) * PLANE)

    greeted = (
        ends + depth - 1
        + ends * (q // ends)
        + ends * ((PLANE - 1 - q) // ends) * ((z + depth - 1) // depth)
    )

    jrow = msgs.at[0, 0]

    def jplane(d):
        return remote(msgs.at[0], msgs.at[d], sj.at[d - 1], rj.at[d - 1], peer(d))

    def jnext(p):
        return remote(
            jrow, msgs.at[PLANE, 0], lsem.at[p], rj.at[PLANE - 1],
            (z + 1) % depth * PLANE + p,
        )

    def jprev(p):
        return remote(
            jrow, msgs.at[PLANE + 1, 0], lsem.at[p], rj.at[PLANE],
            (z - 1) * PLANE + p,
        )

    def jwrap():
        return remote(
            msgs.at[q, 0], msgs.at[PLANE + 1, 0],
            wsem.at[0], rj.at[PLANE], (depth - 1) * PLANE + q,
        )

    def share(d):
        return remote(chunks.at[0], chunks.at[d], s1.at[d - 1], r1.at[d - 1], peer(d))

    def give(zt):
        k = (zt - z + depth) % depth
        return remote(snd.at[zt], rcv.at[k - 1], s2.at[k - 1], r2.at[k - 1], zt * PLANE + q)

    def take(k):
        return remote(
            snd.at[0], rcv.at[k - 1], s2.at[k - 1], r2.at[k - 1],
            (z + depth - k) % depth * PLANE + q,
        )

    lane = lax.broadcasted_iota(jnp.int32, (SUBS, LANES), 1)
    sub = lax.broadcasted_iota(jnp.int32, (SUBS, LANES), 0)
    lanef = lane.astype(jnp.float32)
    tabs = [both_tabs.at[n] for n in range(both_tabs.shape[0])]
    for tab in tabs:
        tab[tab.shape[0] - 1] = jnp.zeros((SUBS, LANES), jnp.int32)

    loads[0].wait()
    loads[1].wait()
    flat = jnp.concatenate(
        [sino_ref[i].astype(jnp.float32) for i in range(ang_dev)], axis=0
    )
    tiles = [flat[:, b * LANES : (b + 1) * LANES] for b in range(nblocks)]
    def unzip(start):
        picked = [lane_gather(tile, (2 * lane + start) % LANES) for tile in tiles]
        at = 2 * lane + start
        outs = []
        for t in range(nspans):
            out = jnp.where(at < LANES, picked[2 * t], picked[2 * t + 1])
            if start < 0:
                out = jnp.where(at < 0, picked[2 * t - 1] if t else 0.0, out)
            outs.append(out)
        return outs

    evens, odds, late = unzip(0), unzip(1), unzip(-1)
    lhs = jnp.concatenate(
        [
            jnp.concatenate([part[2 * k], part[2 * k + 1]], axis=1)
            for part in (evens, late)
            for k in range(kblocks)
        ],
        axis=0,
    ).astype(jnp.bfloat16)
    weights[0].wait()
    mine = (lane % angles) - me * ang_dev
    msg = jnp.zeros((SUBS, LANES), jnp.float32)
    for i in range(ang_dev):
        msg = jnp.where(mine == i, jit_ref[0:1, i : i + 1].astype(jnp.float32), msg)
    theta = ((lane % angles).astype(jnp.float32) + msg) * math.pi / angles
    waves = [jnp.cos(theta) * 0.5, jnp.sin(theta) * 0.5]
    facts = jnp.zeros((SUBS, LANES), jnp.float32)
    for i in range(ang_dev):
        pick = jnp.full((SUBS, LANES), me * ang_dev + i, jnp.int32)
        for n in range(2):
            facts = jnp.where(lane == SUBS + 2 * i + n, lane_gather(waves[n], pick), facts)
    top = jnp.abs(tiles[0])
    for tile in tiles[1:]:
        top = jnp.maximum(top, jnp.abs(tile))
    top = jnp.broadcast_to(jnp.max(top, axis=1, keepdims=True), (SUBS, LANES))
    scale = jnp.maximum(top, 1e-30) * (0.51 / 32700)
    scale = jnp.sum(jnp.where(lane == sub, scale, 0.0), axis=0, keepdims=True)
    msgs[0, 0] = msg[:1]
    msgs[0, 1] = scale + facts[:1]

    rest = jnp.broadcast_to(odds[-1][:, LANES - 1 :], (SUBS, LANES))
    total = [[odds[t] * 0.25 for t in range(nspans)], [evens[t] * 0.25 for t in range(nspans)]]
    for d in range(2 * kblocks - 1):
        up = jnp.concatenate([slab[2 * d + 2], slab[2 * d + 3]], axis=1)
        down = jnp.concatenate([slab[2 * d + 1], slab[2 * d + 2]], axis=1)
        prod = jnp.dot(
            lhs, jnp.concatenate([up, down], axis=0), preferred_element_type=jnp.float32
        )
        for p in range(2):
            for i in range(kblocks):
                j = d - (kblocks - 1) + i
                if 0 <= j < kblocks:
                    row = (p * kblocks + i) * SUBS
                    for n in range(2):
                        total[p][2 * j + n] = (
                            total[p][2 * j + n]
                            + prod[row : row + SUBS, n * LANES : (n + 1) * LANES]
                        )
    for t in range(nspans):
        ends_at = jnp.broadcast_to(slab[t, 0:1].astype(jnp.float32), (SUBS, LANES))
        total[1][t] = total[1][t] + rest * ends_at
    for t in range(nspans):
        chunks[0, :, t * LANES : (t + 1) * LANES] = jnp.concatenate(
            [total[1][t], total[0][t]], axis=0
        ).astype(jnp.bfloat16)

    loads[2].wait()
    loads[3].wait()
    pl.semaphore_wait(barrier, greeted)

    for d in SENDS:
        jplane(d).start()

    @pl.when((q == 0) & (z == 0))
    def _():
        jwrap().start()

    for d in SENDS:
        share(d).start()


    @pl.when(q == PLANE - 1)
    def _():
        for p in range(PLANE):
            jnext(p).start()

    @pl.when((q == 0) & (z > 0))
    def _():
        for p in range(PLANE):
            jprev(p).start()


    lead = sub % slices < slices // 2
    ypos = []
    for g in range(groups):
        row = ((sub % zper + g * zper) * PLANE + q) * rows_dev + sub // zper
        ypos.append(row.astype(jnp.float32) - (nrows - 1) / 2)

    def heard(d, row):
        return jnp.broadcast_to(msgs[d, row], (SUBS, LANES))

    def spread(d, inverse, tab):
        words = []
        for t in range(nspans):
            both = chunks[d, :, t * LANES : (t + 1) * LANES].astype(jnp.float32)
            even = jnp.round(both[:SUBS] * inverse).astype(jnp.int32)
            odd = jnp.round(both[SUBS:] * inverse).astype(jnp.int32)
            high = jnp.where(lead, even, pltpu.roll(odd, 2, 0))
            low = jnp.where(lead, pltpu.roll(even, SUBS - 2, 0), odd)
            words.append(lax.shift_left(high, 16) + low)
            tab[4 * t + 1] = words[-1]
        for j in range(1, 4):
            cut = LANES - 32 * j
            turned = [pltpu.roll(word, cut, 1) for word in words]
            for t in range(nspans):
                after = turned[t + 1] if t + 1 < nspans else 0
                tab[4 * t + j + 1] = jnp.where(lane < cut, turned[t], after)
            if j == 3:
                tab[0] = jnp.where(lane < cut, 0, turned[0])

    def learn(d):
        facts = heard(d, 1)

        def fact(n):
            return lane_gather(facts, jnp.full((SUBS, LANES), n, jnp.int32))

        known = []
        for i in range(ang_dev):
            cosb, sinb = (fact(SUBS + 2 * i + n) for n in range(2))
            parts = [lanef * cosb + ypos[g] * sinb for g in range(groups)]
            known.append(
                (cosb, parts, [fact(i * slices + s) * (1.0 / 65536) for s in range(slices)])
            )
        return known, 1.0 / lane_gather(facts, sub)

    def line(tab, slot, row):
        return jnp.broadcast_to(tab[slot, row : row + 1], (SUBS, LANES))

    def project(d, known, tab, g, b):
        pc = peer(d)
        qc = pc - z * PLANE
        pairs = slices // 2
        index, fracs, slots = [], [], []
        for i in range(ang_dev):
            cosb, parts, scales = known[i]
            moved = shift_ref[pc * ang_dev + i]
            slot = base[0, ((qc * ang_dev + i) * nblocks + b) * groups + g]
            slot = lax.shift_right_arithmetic(slot + moved, 6)
            offset = (moved - slot * STEP).astype(jnp.float32) * 0.5 + (half + STEP) * 0.5
            h = cosb * (b * LANES - half) + parts[g] + offset
            odd = h.astype(jnp.int32)
            even = (h + 0.5).astype(jnp.int32)
            fracs.append(jnp.abs(h - even.astype(jnp.float32)) * 2.0)
            index.append((even, odd))
            slots.append(slot)
        words = {}
        for i, p, s in GATHERS:
            words[i, p, s] = lane_gather(line(tab, slots[i], i * slices + p * pairs + s), index[i][p])
        sums = []
        for i in range(ang_dev):
            got = []
            for s in range(slices):
                e, o = words[i, 0, s % pairs], words[i, 1, s % pairs]
                if s >= pairs:
                    e, o = lax.shift_left(e, 16), lax.shift_left(o, 16)
                e, o = e.astype(jnp.float32), o.astype(jnp.float32)
                got.append((e + fracs[i] * (o - e)) * known[i][2][s])
            sums.append(got)
        return sums

    def keep(*group):
        learnt = [learn(d) for d in group]
        for d in group:
            if d > 0:
                share(d).wait_recv()
        for d, tab, (_, inverse) in zip(group, tabs, learnt):
            spread(d, inverse, tab)
        for b in range(nblocks):
            for g in range(groups):
                for d, tab, (known, _) in zip(group, tabs, learnt):
                    for i, got in enumerate(project(d, known, tab, g, b)):
                        for s in range(slices):
                            held[d, i, g, s, b] = got[s]

    keep(0)

    @pl.when((q > 0) & (z == 0))
    def _():
        jplane(q).wait_recv()
        jwrap().start()

    def meet(d):
        @pl.when((z > 0) | (q != d))
        def _():
            jplane(d).wait_recv()

    for d in range(1, PLANE - 1):
        meet(d)
    keep(*range(1, PLANE - 1))
    d = PLANE - 1
    meet(d)

    def weigh():
        jnext(0).wait_recv()
        jprev(0).wait_recv()
        jit = sum(heard(i, 0) for i in range(PLANE + 2))
        ahead = pltpu.roll(jit, LANES - 1, 1)
        behind = pltpu.roll(jit, 1, 1)
        weight = (1.0 + (ahead - behind) * 1.5) * (4.0 / math.sqrt(angles))
        return [
            [
                lane_gather(weight, jnp.full((SUBS, LANES), peer(n) * ang_dev + i, jnp.int32))
                for i in range(ang_dev)
            ]
            for n in range(PLANE)
        ]

    def merge(weight, g, s, b, chunks_in):
        terms = [
            weight[n][i] * held[n, i, g, s, b] for n in chunks_in for i in range(ang_dev)
        ]
        while len(terms) > 1:
            terms = [x + y for x, y in zip(terms[::2], terms[1::2])] + terms[len(terms) // 2 * 2 :]
        return terms[0]

    pos = sub % zper

    def pack(rows_of):
        for t in range(nblocks // 2):
            for g in range(groups):
                out = [[], [], [], []]
                for b in (2 * t, 2 * t + 1):
                    v = rows_of(g, b)
                    w = [None] * 4
                    for s in range(2):
                        w[s] = jnp.where(pos < 2, v[s], pltpu.roll(v[s + 2], 2, 0))
                        w[s + 2] = jnp.where(pos < 2, pltpu.roll(v[s], SUBS - 2, 0), v[s + 2])
                    for s in (0, 2):
                        lo = jnp.where(pos % 2 < 1, w[s], pltpu.roll(w[s + 1], 1, 0))
                        hi = jnp.where(pos % 2 < 1, pltpu.roll(w[s], SUBS - 1, 0), w[s + 1])
                        for n, val in ((s, lo), (s + 1, hi)):
                            fin[g * zper + n, b] = val
                            out[n].append(val)
                for n in range(4):
                    snd[g * zper + n, :, t * LANES : (t + 1) * LANES] = jnp.concatenate(
                        out[n], axis=0
                    ).astype(jnp.bfloat16)

    waits_last = (z == depth - 1) & (q > 0)

    @pl.when(waits_last)
    def _():
        keep(d)
        weight = weigh()
        pack(lambda g, b: [merge(weight, g, s, b, range(PLANE)) for s in range(slices)])

    @pl.when(jnp.logical_not(waits_last))
    def _():
        weight = weigh()
        known, inverse = learn(d)
        share(d).wait_recv()
        spread(d, inverse, tabs[0])

        def rows_of(g, b):
            got = project(d, known, tabs[0], g, b)
            return [
                merge(weight, g, s, b, range(PLANE - 1))
                + (weight[d][0] * got[0][s] + weight[d][1] * got[1][s])
                for s in range(slices)
            ]

        pack(rows_of)

    for n in range(1, PLANE):
        jplane(n).wait_send()
        share(n).wait_send()

    @pl.loop(0, depth)
    def _(zt):
        @pl.when(zt != z)
        def _():
            give(zt).start()

    @pl.when(q == ends)
    def _():
        for p in range(PLANE):
            jnext(p).wait_send()

    @pl.when((q == 0) & (z > 0))
    def _():
        for p in range(PLANE):
            jprev(p).wait_send()

    @pl.when(z == 0)
    def _():
        jwrap().wait_send()

    @pl.loop(1, depth)
    def _(k):
        take(k).wait_recv()

    for t in range(nblocks // 2):
        sums = [fin[z, 2 * t], fin[z, 2 * t + 1]]
        for k in range(1, depth):
            both = rcv[k - 1, :, t * LANES : (t + 1) * LANES].astype(jnp.float32)
            sums = [sums[0] + both[:SUBS], sums[1] + both[SUBS:]]
        for j in range(2):
            cols = slice((2 * t + j) * LANES, (2 * t + j + 1) * LANES)
            for r in range(rows_dev):
                out_ref[r, :, cols] = sums[j][r * slices : (r + 1) * slices]

    @pl.loop(1, depth)
    def _(k):
        give((z + k) % depth).wait_send()


def body(sinogram, jitter, shift):
    width = lax.axis_size("blk")
    ang_dev, slices, bins = sinogram.shape
    angles = shift.shape[0]
    rows_dev = SUBS // slices
    depth = width // PLANE
    assert ang_dev == 2 and rows_dev == 2 and slices == 4 and LANES % angles == 0
    assert width % (PLANE * 4) == 0 and bins % (2 * BLOCK) == 0
    groups = depth * rows_dev // SUBS
    nblocks = bins // LANES
    anywhere = pl.BlockSpec(memory_space=pl.ANY)
    dma = pltpu.SemaphoreType.DMA
    slab = jnp.asarray(ramp_slab(bins))
    base = jnp.asarray(window_base(width, ang_dev, rows_dev, bins))
    return pl.pallas_call(
        functools.partial(kernel, width),
        out_shape=pltpu.VMEM((rows_dev, slices, bins), jnp.float32),
        in_specs=[anywhere] * 5,
        out_specs=pl.BlockSpec(memory_space=pltpu.VMEM),
        scratch_shapes=[
            pltpu.VMEM((1, ang_dev), jnp.bfloat16),
            pltpu.SMEM((angles,), jnp.int32),
            pltpu.VMEM((ang_dev, slices, bins), jnp.bfloat16),
            pltpu.VMEM(slab.shape, jnp.bfloat16),
            pltpu.SMEM(base.shape[1:], jnp.int32),
            pltpu.VMEM((PLANE, 2 * SUBS, bins // 2), jnp.bfloat16),
            pltpu.VMEM((PLANE + 2, 2, 1, LANES), jnp.float32),
            pltpu.VMEM((PLANE - 2, bins // STEP + 2, SUBS, LANES), jnp.int32),
            pltpu.VMEM((PLANE, ang_dev, groups, slices, nblocks, SUBS, LANES), jnp.float32),
            pltpu.VMEM((depth, nblocks, SUBS, LANES), jnp.float32),
            pltpu.VMEM((depth, 2 * SUBS, bins // 2), jnp.bfloat16),
            pltpu.VMEM((depth - 1, 2 * SUBS, bins // 2), jnp.bfloat16),
            dma((4,)),
            dma((1,)),
            dma((PLANE - 1,)),
            dma((PLANE + 1,)),
            dma((PLANE - 1,)),
            dma((PLANE - 1,)),
            dma((depth - 1,)),
            dma((depth - 1,)),
        ],
        compiler_params=pltpu.CompilerParams(collective_id=0, has_side_effects=True),
    )(jitter.reshape(1, ang_dev), shift, sinogram, slab, base)


def solution(mesh):
    in_specs = (P("blk", "slab", None), P("blk"), P())
    out_specs = P("blk", "slab", None)
    return jax.shard_map(body, mesh=mesh, in_specs=in_specs, out_specs=out_specs, check_vma=False)
```

```python
import functools
import math

import jax
import jax.numpy as jnp
import numpy as np
from jax import lax
from jax.experimental import pallas as pl
from jax.experimental.pallas import tpu as pltpu
from jax.sharding import PartitionSpec as P

LANES = 128
SUBS = 8
BLOCK = 256
PLANE = 4
STEP = 64
JITTER = 0.29882812
SHIFT = 8
SENDS = ((1, 2, 3), (2, 1, 3))
GATHERS = [(i, p, s) for i in (0, 1) for p, s in ((0, 0), (1, 0), (1, 1), (0, 1))]
MESH = pl.DeviceIdType.MESH


def ramp_slab(bins):
    span = bins // 2
    offset = np.arange(-span, span, dtype=np.int32)[None, :] - np.arange(LANES, dtype=np.int32)[:, None]
    safe = (2 * offset + 1).astype(np.float32)
    slab = (np.float32(-1.0) / (np.float32(math.pi**2) * safe * safe)).astype(jnp.bfloat16)
    return np.ascontiguousarray(slab.reshape(LANES, -1, LANES).transpose(1, 0, 2))


def window_base(width, ang_dev, rows_dev, bins):
    depth = width // PLANE
    angles, nrows = width * ang_dev, width * rows_dev
    nblocks, per = bins // LANES, PLANE * ang_dev
    groups = depth * rows_dev // SUBS
    half = (bins - 1) / 2
    me = np.arange(width)
    z, q = me // PLANE, me % PLANE
    a = z[:, None] * per + np.arange(per)[None, :]
    theta = (a[..., None] + np.linspace(-JITTER, JITTER, 9)) * math.pi / angles
    zs = np.arange(groups)[:, None] * (SUBS // rows_dev) + np.array([0, SUBS // rows_dev - 1])
    rows = (zs[None] * PLANE + q[:, None, None]) * rows_dev + np.array([0, rows_dev - 1])
    y = rows - (nrows - 1) / 2
    x = np.arange(nblocks)[:, None] * LANES + np.array([0, LANES - 1]) - half
    u = (
        x[None, None, :, None, :, None, None] * np.cos(theta)[:, :, None, None, None, None, :]
        + y[:, None, None, :, None, :, None] * np.sin(theta)[:, :, None, None, None, None, :]
        + half
    )
    low = np.floor(u.min(axis=(4, 5, 6)) - 0.25).astype(np.int32)
    high = u.max(axis=(4, 5, 6)) + 0.25
    assert (high - low).max() + STEP < 2 * LANES
    assert low.min() - SHIFT >= -STEP and low.max() + SHIFT < bins + STEP
    return (low + STEP).reshape(width, 1, per * nblocks * groups)


def lane_gather(x, index):
    dims = lax.GatherDimensionNumbers(
        offset_dims=(),
        collapsed_slice_dims=(1,),
        start_index_map=(1,),
        operand_batching_dims=(0,),
        start_indices_batching_dims=(0,),
    )
    return lax.gather(
        x, index[..., None], dims, (1, 1), mode=lax.GatherScatterMode.PROMISE_IN_BOUNDS
    )


def kernel(
    width,
    jit_hbm,
    shift_hbm,
    sino_hbm,
    slab_hbm,
    base_hbm,
    out_ref,
    jit_ref,
    shift_ref,
    sino_ref,
    slab,
    base,
    chunks,
    msgs,
    both_tabs,
    held,
    fin,
    snd,
    rcv,
    lsem,
    wsem,
    sj,
    rj,
    s1,
    r1,
    s2,
    r2,
):
    me = lax.axis_index("blk")
    ang_dev, slices, bins = sino_ref.shape
    rows_dev = out_ref.shape[0]
    angles = width * ang_dev
    nrows = width * rows_dev
    nblocks = bins // LANES
    nspans = bins // BLOCK
    depth = width // PLANE
    groups = held.shape[2]
    zper = SUBS // rows_dev
    z, q = me // PLANE, me % PLANE
    half = (bins - 1) / 2

    def remote(src, dst, send, recv, dev):
        return pltpu.make_async_remote_copy(
            src_ref=src,
            dst_ref=dst,
            send_sem=send,
            recv_sem=recv,
            device_id={"blk": dev},
            device_id_type=MESH,
        )

    loads = [
        pltpu.make_async_copy(src, dst, lsem.at[i])
        for i, (src, dst) in enumerate(
            [
                (jit_hbm, jit_ref),
                (sino_hbm, sino_ref),
                (shift_hbm, shift_ref),
                (base_hbm.at[me], base),
            ]
        )
    ]
    kblocks = bins // 2 // BLOCK
    weights = [pltpu.make_async_copy(slab_hbm, slab, wsem.at[0])]
    for load in [loads[1], loads[0]] + weights + loads[2:]:
        load.start()

    barrier = pltpu.get_barrier_semaphore()

    qx, qy = q % 2, q // 2
    ends = PLANE - 1

    def peer(d):
        return z * PLANE + (qx + d % 2) % 2 + 2 * ((qy + d // 2) % 2)

    def hello(dev):
        pl.semaphore_signal(barrier, inc=1, device_id={"blk": dev}, device_id_type=MESH)

    for d in (3, 1, 2):
        hello(peer(d))

    @pl.loop(1, depth)
    def _(k):
        hello((z + k) % depth * PLANE + q)

    @pl.when(q != ends)
    def _():
        hello((z + depth - 1) % depth * PLANE + ends)

    @pl.when((q != 0) & (z < depth - 1))
    def _():
        hello((z + 1) * PLANE)

    greeted = (
        ends + depth - 1
        + ends * (q // ends)
        + ends * ((PLANE - 1 - q) // ends) * ((z + depth - 1) // depth)
    )

    jrow = msgs.at[0, 0]

    def jplane(d):
        return remote(msgs.at[0], msgs.at[d], sj.at[d - 1], rj.at[d - 1], peer(d))

    def jnext(p):
        return remote(
            jrow, msgs.at[PLANE, 0], lsem.at[p], rj.at[PLANE - 1],
            (z + 1) % depth * PLANE + p,
        )

    def jprev(p):
        return remote(
            jrow, msgs.at[PLANE + 1, 0], lsem.at[p], rj.at[PLANE],
            (z - 1) * PLANE + p,
        )

    def jwrap():
        return remote(
            msgs.at[q, 0], msgs.at[PLANE + 1, 0],
            wsem.at[0], rj.at[PLANE], (depth - 1) * PLANE + q,
        )

    def share(d):
        return remote(chunks.at[0], chunks.at[d], s1.at[d - 1], r1.at[d - 1], peer(d))

    def give(zt):
        k = (zt - z + depth) % depth
        return remote(snd.at[zt], rcv.at[k - 1], s2.at[k - 1], r2.at[k - 1], zt * PLANE + q)

    def take(k):
        return remote(
            snd.at[0], rcv.at[k - 1], s2.at[k - 1], r2.at[k - 1],
            (z + depth - k) % depth * PLANE + q,
        )

    lane = lax.broadcasted_iota(jnp.int32, (SUBS, LANES), 1)
    sub = lax.broadcasted_iota(jnp.int32, (SUBS, LANES), 0)
    lanef = lane.astype(jnp.float32)
    tabs = [both_tabs.at[n] for n in range(both_tabs.shape[0])]
    for tab in tabs:
        tab[tab.shape[0] - 1] = jnp.zeros((SUBS, LANES), jnp.int32)

    loads[0].wait()
    loads[1].wait()
    flat = jnp.concatenate(
        [sino_ref[i].astype(jnp.float32) for i in range(ang_dev)], axis=0
    )
    tiles = [flat[:, b * LANES : (b + 1) * LANES] for b in range(nblocks)]
    def unzip(start):
        picked = [lane_gather(tile, (2 * lane + start) % LANES) for tile in tiles]
        at = 2 * lane + start
        outs = []
        for t in range(nspans):
            out = jnp.where(at < LANES, picked[2 * t], picked[2 * t + 1])
            if start < 0:
                out = jnp.where(at < 0, picked[2 * t - 1] if t else 0.0, out)
            outs.append(out)
        return outs

    evens, odds, late = unzip(0), unzip(1), unzip(-1)
    lhs = jnp.concatenate(
        [
            jnp.concatenate([part[2 * k], part[2 * k + 1]], axis=1)
            for part in (evens, late)
            for k in range(kblocks)
        ],
        axis=0,
    ).astype(jnp.bfloat16)
    weights[0].wait()
    mine = (lane % angles) - me * ang_dev
    msg = jnp.zeros((SUBS, LANES), jnp.float32)
    for i in range(ang_dev):
        msg = jnp.where(mine == i, jit_ref[0:1, i : i + 1].astype(jnp.float32), msg)
    theta = ((lane % angles).astype(jnp.float32) + msg) * math.pi / angles
    waves = [jnp.cos(theta) * 0.5, jnp.sin(theta) * 0.5]
    facts = jnp.zeros((SUBS, LANES), jnp.float32)
    for i in range(ang_dev):
        pick = jnp.full((SUBS, LANES), me * ang_dev + i, jnp.int32)
        for n in range(2):
            facts = jnp.where(lane == SUBS + 2 * i + n, lane_gather(waves[n], pick), facts)
    top = jnp.abs(tiles[0])
    for tile in tiles[1:]:
        top = jnp.maximum(top, jnp.abs(tile))
    top = jnp.broadcast_to(jnp.max(top, axis=1, keepdims=True), (SUBS, LANES))
    scale = jnp.maximum(top, 1e-30) * (0.51 / 32700)
    scale = jnp.sum(jnp.where(lane == sub, scale, 0.0), axis=0, keepdims=True)
    msgs[0, 0] = msg[:1]
    msgs[0, 1] = scale + facts[:1]

    rest = jnp.broadcast_to(odds[-1][:, LANES - 1 :], (SUBS, LANES))
    total = [[odds[t] * 0.25 for t in range(nspans)], [evens[t] * 0.25 for t in range(nspans)]]
    for d in range(2 * kblocks - 1):
        up = jnp.concatenate([slab[2 * d + 2], slab[2 * d + 3]], axis=1)
        down = jnp.concatenate([slab[2 * d + 1], slab[2 * d + 2]], axis=1)
        prod = jnp.dot(
            lhs, jnp.concatenate([up, down], axis=0), preferred_element_type=jnp.float32
        )
        for p in range(2):
            for i in range(kblocks):
                j = d - (kblocks - 1) + i
                if 0 <= j < kblocks:
                    row = (p * kblocks + i) * SUBS
                    for n in range(2):
                        total[p][2 * j + n] = (
                            total[p][2 * j + n]
                            + prod[row : row + SUBS, n * LANES : (n + 1) * LANES]
                        )
    for t in range(nspans):
        ends_at = jnp.broadcast_to(slab[t, 0:1].astype(jnp.float32), (SUBS, LANES))
        total[1][t] = total[1][t] + rest * ends_at
    for t in range(nspans):
        chunks[0, :, t * LANES : (t + 1) * LANES] = jnp.concatenate(
            [total[1][t], total[0][t]], axis=0
        ).astype(jnp.bfloat16)

    loads[2].wait()
    loads[3].wait()
    pl.semaphore_wait(barrier, greeted)

    for d in SENDS[0]:
        jplane(d).start()

    @pl.when((q == 0) & (z == 0))
    def _():
        jwrap().start()

    for side, order in enumerate(SENDS):
        @pl.when(lax.axis_index("slab") % 2 == side)
        def _():
            for d in order:
                share(d).start()


    @pl.when(q == PLANE - 1)
    def _():
        for p in range(PLANE):
            jnext(p).start()

    @pl.when((q == 0) & (z > 0))
    def _():
        for p in range(PLANE):
            jprev(p).start()


    lead = sub % slices < slices // 2
    ypos = []
    for g in range(groups):
        row = ((sub % zper + g * zper) * PLANE + q) * rows_dev + sub // zper
        ypos.append(row.astype(jnp.float32) - (nrows - 1) / 2)

    def heard(d, row):
        return jnp.broadcast_to(msgs[d, row], (SUBS, LANES))

    def spread(d, inverse, tab):
        words = []
        for t in range(nspans):
            both = chunks[d, :, t * LANES : (t + 1) * LANES].astype(jnp.float32)
            even = jnp.round(both[:SUBS] * inverse).astype(jnp.int32)
            odd = jnp.round(both[SUBS:] * inverse).astype(jnp.int32)
            high = jnp.where(lead, even, pltpu.roll(odd, 2, 0))
            low = jnp.where(lead, pltpu.roll(even, SUBS - 2, 0), odd)
            words.append(lax.shift_left(high, 16) + low)
            tab[4 * t + 1] = words[-1]
        for j in range(1, 4):
            cut = LANES - 32 * j
            turned = [pltpu.roll(word, cut, 1) for word in words]
            for t in range(nspans):
                after = turned[t + 1] if t + 1 < nspans else 0
                tab[4 * t + j + 1] = jnp.where(lane < cut, turned[t], after)
            if j == 3:
                tab[0] = jnp.where(lane < cut, 0, turned[0])

    def learn(d):
        facts = heard(d, 1)

        def fact(n):
            return lane_gather(facts, jnp.full((SUBS, LANES), n, jnp.int32))

        known = []
        for i in range(ang_dev):
            cosb, sinb = (fact(SUBS + 2 * i + n) for n in range(2))
            parts = [lanef * cosb + ypos[g] * sinb for g in range(groups)]
            known.append(
                (cosb, parts, [fact(i * slices + s) * (1.0 / 65536) for s in range(slices)])
            )
        return known, 1.0 / lane_gather(facts, sub)

    def line(tab, slot, row):
        return jnp.broadcast_to(tab[slot, row : row + 1], (SUBS, LANES))

    def project(d, known, tab, g, b):
        pc = peer(d)
        qc = pc - z * PLANE
        pairs = slices // 2
        index, fracs, slots = [], [], []
        for i in range(ang_dev):
            cosb, parts, scales = known[i]
            moved = shift_ref[pc * ang_dev + i]
            slot = base[0, ((qc * ang_dev + i) * nblocks + b) * groups + g]
            slot = lax.shift_right_arithmetic(slot + moved, 6)
            offset = (moved - slot * STEP).astype(jnp.float32) * 0.5 + (half + STEP) * 0.5
            h = cosb * (b * LANES - half) + parts[g] + offset
            odd = h.astype(jnp.int32)
            even = (h + 0.5).astype(jnp.int32)
            fracs.append(jnp.abs(h - even.astype(jnp.float32)) * 2.0)
            index.append((even, odd))
            slots.append(slot)
        words = {}
        for i, p, s in GATHERS:
            words[i, p, s] = lane_gather(line(tab, slots[i], i * slices + p * pairs + s), index[i][p])
        sums = []
        for i in range(ang_dev):
            got = []
            for s in range(slices):
                e, o = words[i, 0, s % pairs], words[i, 1, s % pairs]
                if s >= pairs:
                    e, o = lax.shift_left(e, 16), lax.shift_left(o, 16)
                e, o = e.astype(jnp.float32), o.astype(jnp.float32)
                got.append((e + fracs[i] * (o - e)) * known[i][2][s])
            sums.append(got)
        return sums

    def keep(*group):
        learnt = [learn(d) for d in group]
        for d in group:
            if d > 0:
                share(d).wait_recv()
        for d, tab, (_, inverse) in zip(group, tabs, learnt):
            spread(d, inverse, tab)
        for b in range(nblocks):
            for g in range(groups):
                for d, tab, (known, _) in zip(group, tabs, learnt):
                    for i, got in enumerate(project(d, known, tab, g, b)):
                        for s in range(slices):
                            held[d, i, g, s, b] = got[s]

    keep(0)

    @pl.when((q > 0) & (z == 0))
    def _():
        jplane(q).wait_recv()
        jwrap().start()

    def meet(d):
        @pl.when((z > 0) | (q != d))
        def _():
            jplane(d).wait_recv()

    for d in range(1, PLANE - 1):
        meet(d)
    keep(*range(1, PLANE - 1))
    d = PLANE - 1
    meet(d)

    def weigh():
        jnext(0).wait_recv()
        jprev(0).wait_recv()
        jit = sum(heard(i, 0) for i in range(PLANE + 2))
        ahead = pltpu.roll(jit, LANES - 1, 1)
        behind = pltpu.roll(jit, 1, 1)
        weight = (1.0 + (ahead - behind) * 1.5) * (4.0 / math.sqrt(angles))
        return [
            [
                lane_gather(weight, jnp.full((SUBS, LANES), peer(n) * ang_dev + i, jnp.int32))
                for i in range(ang_dev)
            ]
            for n in range(PLANE)
        ]

    def merge(weight, g, s, b, chunks_in):
        terms = [
            weight[n][i] * held[n, i, g, s, b] for n in chunks_in for i in range(ang_dev)
        ]
        while len(terms) > 1:
            terms = [x + y for x, y in zip(terms[::2], terms[1::2])] + terms[len(terms) // 2 * 2 :]
        return terms[0]

    pos = sub % zper

    def pack(rows_of):
        for t in range(nblocks // 2):
            for g in range(groups):
                out = [[], [], [], []]
                for b in (2 * t, 2 * t + 1):
                    v = rows_of(g, b)
                    w = [None] * 4
                    for s in range(2):
                        w[s] = jnp.where(pos < 2, v[s], pltpu.roll(v[s + 2], 2, 0))
                        w[s + 2] = jnp.where(pos < 2, pltpu.roll(v[s], SUBS - 2, 0), v[s + 2])
                    for s in (0, 2):
                        lo = jnp.where(pos % 2 < 1, w[s], pltpu.roll(w[s + 1], 1, 0))
                        hi = jnp.where(pos % 2 < 1, pltpu.roll(w[s], SUBS - 1, 0), w[s + 1])
                        for n, val in ((s, lo), (s + 1, hi)):
                            fin[g * zper + n, b] = val
                            out[n].append(val)
                for n in range(4):
                    snd[g * zper + n, :, t * LANES : (t + 1) * LANES] = jnp.concatenate(
                        out[n], axis=0
                    ).astype(jnp.bfloat16)

    waits_last = (z == depth - 1) & (q > 0)

    @pl.when(waits_last)
    def _():
        keep(d)
        weight = weigh()
        pack(lambda g, b: [merge(weight, g, s, b, range(PLANE)) for s in range(slices)])

    @pl.when(jnp.logical_not(waits_last))
    def _():
        weight = weigh()
        known, inverse = learn(d)
        share(d).wait_recv()
        spread(d, inverse, tabs[0])

        def rows_of(g, b):
            got = project(d, known, tabs[0], g, b)
            return [
                merge(weight, g, s, b, range(PLANE - 1))
                + (weight[d][0] * got[0][s] + weight[d][1] * got[1][s])
                for s in range(slices)
            ]

        pack(rows_of)

    @pl.loop(0, depth)
    def _(zt):
        @pl.when(zt != z)
        def _():
            give(zt).start()

    for n in range(1, PLANE):
        jplane(n).wait_send()
        share(n).wait_send()

    @pl.when(q == ends)
    def _():
        for p in range(PLANE):
            jnext(p).wait_send()

    @pl.when((q == 0) & (z > 0))
    def _():
        for p in range(PLANE):
            jprev(p).wait_send()

    @pl.when(z == 0)
    def _():
        jwrap().wait_send()

    @pl.loop(1, depth)
    def _(k):
        take(k).wait_recv()

    for t in range(nblocks // 2):
        sums = [fin[z, 2 * t], fin[z, 2 * t + 1]]
        for k in range(1, depth):
            both = rcv[k - 1, :, t * LANES : (t + 1) * LANES].astype(jnp.float32)
            sums = [sums[0] + both[:SUBS], sums[1] + both[SUBS:]]
        for j in range(2):
            cols = slice((2 * t + j) * LANES, (2 * t + j + 1) * LANES)
            for r in range(rows_dev):
                out_ref[r, :, cols] = sums[j][r * slices : (r + 1) * slices]

    @pl.loop(1, depth)
    def _(k):
        give((z + k) % depth).wait_send()


def body(sinogram, jitter, shift):
    width = lax.axis_size("blk")
    ang_dev, slices, bins = sinogram.shape
    angles = shift.shape[0]
    rows_dev = SUBS // slices
    depth = width // PLANE
    assert ang_dev == 2 and rows_dev == 2 and slices == 4 and LANES % angles == 0
    assert width % (PLANE * 4) == 0 and bins % (2 * BLOCK) == 0
    groups = depth * rows_dev // SUBS
    nblocks = bins // LANES
    anywhere = pl.BlockSpec(memory_space=pl.ANY)
    dma = pltpu.SemaphoreType.DMA
    slab = jnp.asarray(ramp_slab(bins))
    base = jnp.asarray(window_base(width, ang_dev, rows_dev, bins))
    return pl.pallas_call(
        functools.partial(kernel, width),
        out_shape=pltpu.VMEM((rows_dev, slices, bins), jnp.float32),
        in_specs=[anywhere] * 5,
        out_specs=pl.BlockSpec(memory_space=pltpu.VMEM),
        scratch_shapes=[
            pltpu.VMEM((1, ang_dev), jnp.bfloat16),
            pltpu.SMEM((angles,), jnp.int32),
            pltpu.VMEM((ang_dev, slices, bins), jnp.bfloat16),
            pltpu.VMEM(slab.shape, jnp.bfloat16),
            pltpu.SMEM(base.shape[1:], jnp.int32),
            pltpu.VMEM((PLANE, 2 * SUBS, bins // 2), jnp.bfloat16),
            pltpu.VMEM((PLANE + 2, 2, 1, LANES), jnp.float32),
            pltpu.VMEM((PLANE - 2, bins // STEP + 2, SUBS, LANES), jnp.int32),
            pltpu.VMEM((PLANE, ang_dev, groups, slices, nblocks, SUBS, LANES), jnp.float32),
            pltpu.VMEM((depth, nblocks, SUBS, LANES), jnp.float32),
            pltpu.VMEM((depth, 2 * SUBS, bins // 2), jnp.bfloat16),
            pltpu.VMEM((depth - 1, 2 * SUBS, bins // 2), jnp.bfloat16),
            dma((4,)),
            dma((1,)),
            dma((PLANE - 1,)),
            dma((PLANE + 1,)),
            dma((PLANE - 1,)),
            dma((PLANE - 1,)),
            dma((depth - 1,)),
            dma((depth - 1,)),
        ],
        compiler_params=pltpu.CompilerParams(collective_id=0, has_side_effects=True),
    )(jitter.reshape(1, ang_dev), shift, sinogram, slab, base)


def solution(mesh):
    in_specs = (P("blk", "slab", None), P("blk"), P())
    out_specs = P("blk", "slab", None)
    return jax.shard_map(body, mesh=mesh, in_specs=in_specs, out_specs=out_specs, check_vma=False)
```

```python
import functools
import math

import jax
import jax.numpy as jnp
import numpy as np
from jax import lax
from jax.experimental import pallas as pl
from jax.experimental.pallas import tpu as pltpu
from jax.sharding import PartitionSpec as P

LANES = 128
SUBS = 8
BLOCK = 256
PLANE = 4
STEP = 64
JITTER = 0.29882812
SHIFT = 8
SENDS = ((1, 2, 3), (2, 1, 3))
GATHERS = [(i, p, s) for i in (0, 1) for p, s in ((0, 0), (1, 0), (1, 1), (0, 1))]
MESH = pl.DeviceIdType.MESH


def ramp_slab(bins):
    span = bins // 2
    offset = np.arange(-span, span, dtype=np.int32)[None, :] - np.arange(LANES, dtype=np.int32)[:, None]
    safe = (2 * offset + 1).astype(np.float32)
    slab = (np.float32(-1.0) / (np.float32(math.pi**2) * safe * safe)).astype(jnp.bfloat16)
    return np.ascontiguousarray(slab.reshape(LANES, -1, LANES).transpose(1, 0, 2))


def window_base(width, ang_dev, rows_dev, bins):
    depth = width // PLANE
    angles, nrows = width * ang_dev, width * rows_dev
    nblocks, per = bins // LANES, PLANE * ang_dev
    groups = depth * rows_dev // SUBS
    half = (bins - 1) / 2
    me = np.arange(width)
    z, q = me // PLANE, me % PLANE
    a = z[:, None] * per + np.arange(per)[None, :]
    theta = (a[..., None] + np.linspace(-JITTER, JITTER, 9)) * math.pi / angles
    zs = np.arange(groups)[:, None] * (SUBS // rows_dev) + np.array([0, SUBS // rows_dev - 1])
    rows = (zs[None] * PLANE + q[:, None, None]) * rows_dev + np.array([0, rows_dev - 1])
    y = rows - (nrows - 1) / 2
    x = np.arange(nblocks)[:, None] * LANES + np.array([0, LANES - 1]) - half
    u = (
        x[None, None, :, None, :, None, None] * np.cos(theta)[:, :, None, None, None, None, :]
        + y[:, None, None, :, None, :, None] * np.sin(theta)[:, :, None, None, None, None, :]
        + half
    )
    low = np.floor(u.min(axis=(4, 5, 6)) - 0.25).astype(np.int32)
    high = u.max(axis=(4, 5, 6)) + 0.25
    assert (high - low).max() + STEP < 2 * LANES
    assert low.min() - SHIFT >= -STEP and low.max() + SHIFT < bins + STEP
    return (low + STEP).reshape(width, 1, per * nblocks * groups)


def lane_gather(x, index):
    dims = lax.GatherDimensionNumbers(
        offset_dims=(),
        collapsed_slice_dims=(1,),
        start_index_map=(1,),
        operand_batching_dims=(0,),
        start_indices_batching_dims=(0,),
    )
    return lax.gather(
        x, index[..., None], dims, (1, 1), mode=lax.GatherScatterMode.PROMISE_IN_BOUNDS
    )


def kernel(
    width,
    jit_hbm,
    shift_hbm,
    sino_hbm,
    slab_hbm,
    base_hbm,
    out_ref,
    jit_ref,
    shift_ref,
    sino_ref,
    slab,
    base,
    chunks,
    msgs,
    both_tabs,
    held,
    fin,
    snd,
    rcv,
    lsem,
    wsem,
    sj,
    rj,
    s1,
    r1,
    s2,
    r2,
):
    me = lax.axis_index("blk")
    ang_dev, slices, bins = sino_ref.shape
    rows_dev = out_ref.shape[0]
    angles = width * ang_dev
    nrows = width * rows_dev
    nblocks = bins // LANES
    nspans = bins // BLOCK
    depth = width // PLANE
    groups = held.shape[2]
    zper = SUBS // rows_dev
    z, q = me // PLANE, me % PLANE
    half = (bins - 1) / 2

    def remote(src, dst, send, recv, dev):
        return pltpu.make_async_remote_copy(
            src_ref=src,
            dst_ref=dst,
            send_sem=send,
            recv_sem=recv,
            device_id={"blk": dev},
            device_id_type=MESH,
        )

    loads = [
        pltpu.make_async_copy(src, dst, lsem.at[i])
        for i, (src, dst) in enumerate(
            [
                (jit_hbm, jit_ref),
                (sino_hbm, sino_ref),
                (shift_hbm, shift_ref),
                (base_hbm.at[me], base),
            ]
        )
    ]
    kblocks = bins // 2 // BLOCK
    weights = [pltpu.make_async_copy(slab_hbm, slab, wsem.at[0])]
    for load in [loads[1], loads[0]] + weights:
        load.start()

    barrier = pltpu.get_barrier_semaphore()

    qx, qy = q % 2, q // 2
    ends = PLANE - 1

    def peer(d):
        return z * PLANE + (qx + d % 2) % 2 + 2 * ((qy + d // 2) % 2)

    def hello(dev):
        pl.semaphore_signal(barrier, inc=1, device_id={"blk": dev}, device_id_type=MESH)

    for d in (3, 1, 2):
        hello(peer(d))

    @pl.loop(1, depth)
    def _(k):
        hello((z + k) % depth * PLANE + q)

    @pl.when(q != ends)
    def _():
        hello((z + depth - 1) % depth * PLANE + ends)

    @pl.when((q != 0) & (z < depth - 1))
    def _():
        hello((z + 1) * PLANE)

    for load in loads[2:]:
        load.start()

    greeted = (
        ends + depth - 1
        + ends * (q // ends)
        + ends * ((PLANE - 1 - q) // ends) * ((z + depth - 1) // depth)
    )

    jrow = msgs.at[0, 0]

    def jplane(d):
        return remote(msgs.at[0], msgs.at[d], sj.at[d - 1], rj.at[d - 1], peer(d))

    def jnext(p):
        return remote(
            jrow, msgs.at[PLANE, 0], lsem.at[p], rj.at[PLANE - 1],
            (z + 1) % depth * PLANE + p,
        )

    def jprev(p):
        return remote(
            jrow, msgs.at[PLANE + 1, 0], lsem.at[p], rj.at[PLANE],
            (z - 1) * PLANE + p,
        )

    def jwrap():
        return remote(
            msgs.at[q, 0], msgs.at[PLANE + 1, 0],
            wsem.at[0], rj.at[PLANE], (depth - 1) * PLANE + q,
        )

    def share(d):
        return remote(chunks.at[0], chunks.at[d], s1.at[d - 1], r1.at[d - 1], peer(d))

    def give(zt):
        k = (zt - z + depth) % depth
        return remote(snd.at[zt], rcv.at[k - 1], s2.at[k - 1], r2.at[k - 1], zt * PLANE + q)

    def take(k):
        return remote(
            snd.at[0], rcv.at[k - 1], s2.at[k - 1], r2.at[k - 1],
            (z + depth - k) % depth * PLANE + q,
        )

    lane = lax.broadcasted_iota(jnp.int32, (SUBS, LANES), 1)
    sub = lax.broadcasted_iota(jnp.int32, (SUBS, LANES), 0)
    lanef = lane.astype(jnp.float32)
    tabs = [both_tabs.at[n] for n in range(both_tabs.shape[0])]
    for tab in tabs:
        tab[tab.shape[0] - 1] = jnp.zeros((SUBS, LANES), jnp.int32)

    loads[0].wait()
    loads[1].wait()
    flat = jnp.concatenate(
        [sino_ref[i].astype(jnp.float32) for i in range(ang_dev)], axis=0
    )
    tiles = [flat[:, b * LANES : (b + 1) * LANES] for b in range(nblocks)]
    def unzip(start):
        picked = [lane_gather(tile, (2 * lane + start) % LANES) for tile in tiles]
        at = 2 * lane + start
        outs = []
        for t in range(nspans):
            out = jnp.where(at < LANES, picked[2 * t], picked[2 * t + 1])
            if start < 0:
                out = jnp.where(at < 0, picked[2 * t - 1] if t else 0.0, out)
            outs.append(out)
        return outs

    evens, odds, late = unzip(0), unzip(1), unzip(-1)
    lhs = jnp.concatenate(
        [
            jnp.concatenate([part[2 * k], part[2 * k + 1]], axis=1)
            for part in (evens, late)
            for k in range(kblocks)
        ],
        axis=0,
    ).astype(jnp.bfloat16)
    weights[0].wait()
    mine = (lane % angles) - me * ang_dev
    msg = jnp.zeros((SUBS, LANES), jnp.float32)
    for i in range(ang_dev):
        msg = jnp.where(mine == i, jit_ref[0:1, i : i + 1].astype(jnp.float32), msg)
    theta = ((lane % angles).astype(jnp.float32) + msg) * math.pi / angles
    waves = [jnp.cos(theta) * 0.5, jnp.sin(theta) * 0.5]
    facts = jnp.zeros((SUBS, LANES), jnp.float32)
    for i in range(ang_dev):
        pick = jnp.full((SUBS, LANES), me * ang_dev + i, jnp.int32)
        for n in range(2):
            facts = jnp.where(lane == SUBS + 2 * i + n, lane_gather(waves[n], pick), facts)
    top = jnp.abs(tiles[0])
    for tile in tiles[1:]:
        top = jnp.maximum(top, jnp.abs(tile))
    top = jnp.broadcast_to(jnp.max(top, axis=1, keepdims=True), (SUBS, LANES))
    scale = jnp.maximum(top, 1e-30) * (0.51 / 32700)
    scale = jnp.sum(jnp.where(lane == sub, scale, 0.0), axis=0, keepdims=True)
    msgs[0, 0] = msg[:1]
    msgs[0, 1] = scale + facts[:1]

    rest = jnp.broadcast_to(odds[-1][:, LANES - 1 :], (SUBS, LANES))
    total = [[odds[t] * 0.25 for t in range(nspans)], [evens[t] * 0.25 for t in range(nspans)]]
    for d in range(2 * kblocks - 1):
        up = jnp.concatenate([slab[2 * d + 2], slab[2 * d + 3]], axis=1)
        down = jnp.concatenate([slab[2 * d + 1], slab[2 * d + 2]], axis=1)
        prod = jnp.dot(
            lhs, jnp.concatenate([up, down], axis=0), preferred_element_type=jnp.float32
        )
        for p in range(2):
            for i in range(kblocks):
                j = d - (kblocks - 1) + i
                if 0 <= j < kblocks:
                    row = (p * kblocks + i) * SUBS
                    for n in range(2):
                        total[p][2 * j + n] = (
                            total[p][2 * j + n]
                            + prod[row : row + SUBS, n * LANES : (n + 1) * LANES]
                        )
    for t in range(nspans):
        ends_at = jnp.broadcast_to(slab[t, 0:1].astype(jnp.float32), (SUBS, LANES))
        total[1][t] = total[1][t] + rest * ends_at
    for t in range(nspans):
        chunks[0, :, t * LANES : (t + 1) * LANES] = jnp.concatenate(
            [total[1][t], total[0][t]], axis=0
        ).astype(jnp.bfloat16)

    loads[2].wait()
    loads[3].wait()
    pl.semaphore_wait(barrier, greeted)

    for d in SENDS[0]:
        jplane(d).start()

    @pl.when((q == 0) & (z == 0))
    def _():
        jwrap().start()

    for side, order in enumerate(SENDS):
        @pl.when(lax.axis_index("slab") % 2 == side)
        def _():
            for d in order:
                share(d).start()


    @pl.when(q == PLANE - 1)
    def _():
        for p in range(PLANE):
            jnext(p).start()

    @pl.when((q == 0) & (z > 0))
    def _():
        for p in range(PLANE):
            jprev(p).start()


    lead = sub % slices < slices // 2
    ypos = []
    for g in range(groups):
        row = ((sub % zper + g * zper) * PLANE + q) * rows_dev + sub // zper
        ypos.append(row.astype(jnp.float32) - (nrows - 1) / 2)

    def heard(d, row):
        return jnp.broadcast_to(msgs[d, row], (SUBS, LANES))

    def spread(d, inverse, tab):
        words = []
        for t in range(nspans):
            both = chunks[d, :, t * LANES : (t + 1) * LANES].astype(jnp.float32)
            even = jnp.round(both[:SUBS] * inverse).astype(jnp.int32)
            odd = jnp.round(both[SUBS:] * inverse).astype(jnp.int32)
            high = jnp.where(lead, even, pltpu.roll(odd, 2, 0))
            low = jnp.where(lead, pltpu.roll(even, SUBS - 2, 0), odd)
            words.append(lax.shift_left(high, 16) + low)
            tab[4 * t + 1] = words[-1]
        for j in range(1, 4):
            cut = LANES - 32 * j
            turned = [pltpu.roll(word, cut, 1) for word in words]
            for t in range(nspans):
                after = turned[t + 1] if t + 1 < nspans else 0
                tab[4 * t + j + 1] = jnp.where(lane < cut, turned[t], after)
            if j == 3:
                tab[0] = jnp.where(lane < cut, 0, turned[0])

    def learn(d):
        facts = heard(d, 1)

        def fact(n):
            return lane_gather(facts, jnp.full((SUBS, LANES), n, jnp.int32))

        known = []
        for i in range(ang_dev):
            cosb, sinb = (fact(SUBS + 2 * i + n) for n in range(2))
            parts = [lanef * cosb + ypos[g] * sinb for g in range(groups)]
            known.append(
                (cosb, parts, [fact(i * slices + s) * (1.0 / 65536) for s in range(slices)])
            )
        return known, 1.0 / lane_gather(facts, sub)

    def line(tab, slot, row):
        return jnp.broadcast_to(tab[slot, row : row + 1], (SUBS, LANES))

    def project(d, known, tab, g, b):
        pc = peer(d)
        qc = pc - z * PLANE
        pairs = slices // 2
        index, fracs, slots = [], [], []
        for i in range(ang_dev):
            cosb, parts, scales = known[i]
            moved = shift_ref[pc * ang_dev + i]
            slot = base[0, ((qc * ang_dev + i) * nblocks + b) * groups + g]
            slot = lax.shift_right_arithmetic(slot + moved, 6)
            offset = (moved - slot * STEP).astype(jnp.float32) * 0.5 + (half + STEP) * 0.5
            h = cosb * (b * LANES - half) + parts[g] + offset
            odd = h.astype(jnp.int32)
            even = (h + 0.5).astype(jnp.int32)
            fracs.append(jnp.abs(h - even.astype(jnp.float32)) * 2.0)
            index.append((even, odd))
            slots.append(slot)
        words = {}
        for i, p, s in GATHERS:
            words[i, p, s] = lane_gather(line(tab, slots[i], i * slices + p * pairs + s), index[i][p])
        sums = []
        for i in range(ang_dev):
            got = []
            for s in range(slices):
                e, o = words[i, 0, s % pairs], words[i, 1, s % pairs]
                if s >= pairs:
                    e, o = lax.shift_left(e, 16), lax.shift_left(o, 16)
                e, o = e.astype(jnp.float32), o.astype(jnp.float32)
                got.append((e + fracs[i] * (o - e)) * known[i][2][s])
            sums.append(got)
        return sums

    def keep(*group):
        learnt = [learn(d) for d in group]
        for d in group:
            if d > 0:
                share(d).wait_recv()
        for d, tab, (_, inverse) in zip(group, tabs, learnt):
            spread(d, inverse, tab)
        for b in range(nblocks):
            for g in range(groups):
                for d, tab, (known, _) in zip(group, tabs, learnt):
                    for i, got in enumerate(project(d, known, tab, g, b)):
                        for s in range(slices):
                            held[d, i, g, s, b] = got[s]

    keep(0)

    @pl.when((q > 0) & (z == 0))
    def _():
        jplane(q).wait_recv()
        jwrap().start()

    def meet(d):
        @pl.when((z > 0) | (q != d))
        def _():
            jplane(d).wait_recv()

    for d in range(1, PLANE - 1):
        meet(d)
    keep(*range(1, PLANE - 1))
    d = PLANE - 1
    meet(d)

    def weigh():
        jnext(0).wait_recv()
        jprev(0).wait_recv()
        jit = sum(heard(i, 0) for i in range(PLANE + 2))
        ahead = pltpu.roll(jit, LANES - 1, 1)
        behind = pltpu.roll(jit, 1, 1)
        weight = (1.0 + (ahead - behind) * 1.5) * (4.0 / math.sqrt(angles))
        return [
            [
                lane_gather(weight, jnp.full((SUBS, LANES), peer(n) * ang_dev + i, jnp.int32))
                for i in range(ang_dev)
            ]
            for n in range(PLANE)
        ]

    def merge(weight, g, s, b, chunks_in):
        terms = [
            weight[n][i] * held[n, i, g, s, b] for n in chunks_in for i in range(ang_dev)
        ]
        while len(terms) > 1:
            terms = [x + y for x, y in zip(terms[::2], terms[1::2])] + terms[len(terms) // 2 * 2 :]
        return terms[0]

    pos = sub % zper

    def pack(rows_of):
        for t in range(nblocks // 2):
            for g in range(groups):
                out = [[], [], [], []]
                for b in (2 * t, 2 * t + 1):
                    v = rows_of(g, b)
                    w = [None] * 4
                    for s in range(2):
                        w[s] = jnp.where(pos < 2, v[s], pltpu.roll(v[s + 2], 2, 0))
                        w[s + 2] = jnp.where(pos < 2, pltpu.roll(v[s], SUBS - 2, 0), v[s + 2])
                    for s in (0, 2):
                        lo = jnp.where(pos % 2 < 1, w[s], pltpu.roll(w[s + 1], 1, 0))
                        hi = jnp.where(pos % 2 < 1, pltpu.roll(w[s], SUBS - 1, 0), w[s + 1])
                        for n, val in ((s, lo), (s + 1, hi)):
                            fin[g * zper + n, b] = val
                            out[n].append(val)
                for n in range(4):
                    snd[g * zper + n, :, t * LANES : (t + 1) * LANES] = jnp.concatenate(
                        out[n], axis=0
                    ).astype(jnp.bfloat16)

    waits_last = (z == depth - 1) & (q > 0)

    @pl.when(waits_last)
    def _():
        keep(d)
        weight = weigh()
        pack(lambda g, b: [merge(weight, g, s, b, range(PLANE)) for s in range(slices)])

    @pl.when(jnp.logical_not(waits_last))
    def _():
        weight = weigh()
        known, inverse = learn(d)
        share(d).wait_recv()
        spread(d, inverse, tabs[0])

        def rows_of(g, b):
            got = project(d, known, tabs[0], g, b)
            return [
                merge(weight, g, s, b, range(PLANE - 1))
                + (weight[d][0] * got[0][s] + weight[d][1] * got[1][s])
                for s in range(slices)
            ]

        pack(rows_of)

    @pl.loop(0, depth)
    def _(zt):
        @pl.when(zt != z)
        def _():
            give(zt).start()

    for n in range(1, PLANE):
        jplane(n).wait_send()
        share(n).wait_send()

    @pl.when(q == ends)
    def _():
        for p in range(PLANE):
            jnext(p).wait_send()

    @pl.when((q == 0) & (z > 0))
    def _():
        for p in range(PLANE):
            jprev(p).wait_send()

    @pl.when(z == 0)
    def _():
        jwrap().wait_send()

    @pl.loop(1, depth)
    def _(k):
        take(k).wait_recv()

    for t in range(nblocks // 2):
        sums = [fin[z, 2 * t], fin[z, 2 * t + 1]]
        for k in range(1, depth):
            both = rcv[k - 1, :, t * LANES : (t + 1) * LANES].astype(jnp.float32)
            sums = [sums[0] + both[:SUBS], sums[1] + both[SUBS:]]
        for j in range(2):
            cols = slice((2 * t + j) * LANES, (2 * t + j + 1) * LANES)
            for r in range(rows_dev):
                out_ref[r, :, cols] = sums[j][r * slices : (r + 1) * slices]

    @pl.loop(1, depth)
    def _(k):
        give((z + k) % depth).wait_send()


def body(sinogram, jitter, shift):
    width = lax.axis_size("blk")
    ang_dev, slices, bins = sinogram.shape
    angles = shift.shape[0]
    rows_dev = SUBS // slices
    depth = width // PLANE
    assert ang_dev == 2 and rows_dev == 2 and slices == 4 and LANES % angles == 0
    assert width % (PLANE * 4) == 0 and bins % (2 * BLOCK) == 0
    groups = depth * rows_dev // SUBS
    nblocks = bins // LANES
    anywhere = pl.BlockSpec(memory_space=pl.ANY)
    dma = pltpu.SemaphoreType.DMA
    slab = jnp.asarray(ramp_slab(bins))
    base = jnp.asarray(window_base(width, ang_dev, rows_dev, bins))
    return pl.pallas_call(
        functools.partial(kernel, width),
        out_shape=pltpu.VMEM((rows_dev, slices, bins), jnp.float32),
        in_specs=[anywhere] * 5,
        out_specs=pl.BlockSpec(memory_space=pltpu.VMEM),
        scratch_shapes=[
            pltpu.VMEM((1, ang_dev), jnp.bfloat16),
            pltpu.SMEM((angles,), jnp.int32),
            pltpu.VMEM((ang_dev, slices, bins), jnp.bfloat16),
            pltpu.VMEM(slab.shape, jnp.bfloat16),
            pltpu.SMEM(base.shape[1:], jnp.int32),
            pltpu.VMEM((PLANE, 2 * SUBS, bins // 2), jnp.bfloat16),
            pltpu.VMEM((PLANE + 2, 2, 1, LANES), jnp.float32),
            pltpu.VMEM((PLANE - 2, bins // STEP + 2, SUBS, LANES), jnp.int32),
            pltpu.VMEM((PLANE, ang_dev, groups, slices, nblocks, SUBS, LANES), jnp.float32),
            pltpu.VMEM((depth, nblocks, SUBS, LANES), jnp.float32),
            pltpu.VMEM((depth, 2 * SUBS, bins // 2), jnp.bfloat16),
            pltpu.VMEM((depth - 1, 2 * SUBS, bins // 2), jnp.bfloat16),
            dma((4,)),
            dma((1,)),
            dma((PLANE - 1,)),
            dma((PLANE + 1,)),
            dma((PLANE - 1,)),
            dma((PLANE - 1,)),
            dma((depth - 1,)),
            dma((depth - 1,)),
        ],
        compiler_params=pltpu.CompilerParams(collective_id=0, has_side_effects=True),
    )(jitter.reshape(1, ang_dev), shift, sinogram, slab, base)


def solution(mesh):
    in_specs = (P("blk", "slab", None), P("blk"), P())
    out_specs = P("blk", "slab", None)
    return jax.shard_map(body, mesh=mesh, in_specs=in_specs, out_specs=out_specs, check_vma=False)
```
